32 devices in a mesh: depth: 8 (over z, x), rows: 4 (over y, core).
Axes of the slice: x: 2, y: 2, z: 4, core: 2. Of those that a mesh axis runs over, the one named last changes fastest.
Arguments:
- density: float32 [128, 64, 1024], P('depth', 'rows'), may hold values from 0 to 1
- bin_of_level: int32 [16], replicated, may hold values from 0 to 7
- absorb_bins: float32 [8], replicated, may hold values from 0.00234375 to 0.0625
- emit_bins: float32 [8], replicated, may hold values from 0.2 to 3
- occupancy: int32 [8, 4, 8], P('depth', 'rows'), may hold values 0 or 1
- col_offsets: int32 [1024], replicated, may hold values from 2 to 6
- row_offsets: int32 [64], P('rows'), may hold values from 2 to 6
Outputs:
- front_transmittance: float32 [8, 64, 1024], P('depth', 'rows')
- final_image: float32 [2, 64, 1024], P(None, 'rows')
The draws below stay inside these ranges and needn't reach their ends.
All inputs are finite; a program needn't handle non-finite values. No bound on the sum of `occupancy` on one device may be relied on, other than what follows from the above.
Results may differ from the reference program's by a relative error of at most 0.0002.
Values sent between devices are 32-bit elements; how exact they have to be, the bound alone decides.
A program may use at most 64 MiB of HBM per device.

```python
import math
import jax
import jax.numpy as jnp
from jax import lax

COLS = 1024
LEVELS = 16
BINS = 8
SLAB = 16
ROW_DEV = 16
DEPTH_ALL = 128
ROWS_ALL = 64
TILES = 8
N_DEPTH = 8
N_ROWS = 4


def set_ends(entries, rng, smallest, top_value):
    place = [jax.random.randint(jax.random.fold_in(rng, axis), (), 0, length) for axis, length in enumerate(entries.shape)]
    widest = entries.shape.index(max(entries.shape))
    beside = place[:widest] + [(place[widest] + 1) % entries.shape[widest]] + place[widest + 1:]
    return entries.at[tuple(place)].set(smallest).at[tuple(beside)].set(top_value)


def block_scale(rng, shape, shards, least, largest):
    gain, own = 1.0, jax.random.fold_in(rng, 6)
    for axis_at, blocks in shards:
        heights = jnp.exp(jax.random.uniform(jax.random.fold_in(own, axis_at), (blocks,), jnp.float32, least / len(shards), largest / len(shards)))
        gain = gain * jnp.repeat(heights, shape[axis_at] // blocks).reshape([-1 if axis == axis_at else 1 for axis in range(len(shape))])
    return gain


def setup_inputs(seed: int = 0) -> dict:
    key_list = jax.random.split(jax.random.key(seed), 8)
    return {
        "density": jnp.clip(1.0 * jax.random.uniform(key_list[0], (DEPTH_ALL, ROWS_ALL, COLS), jnp.float32) ** block_scale(key_list[0], (DEPTH_ALL, ROWS_ALL, COLS), ((0, 8), (1, 4)), -0.2, 0.2), 0.0, 1.0),
        "bin_of_level": set_ends(jax.random.randint(key_list[1], (LEVELS,), 0, BINS), jax.random.fold_in(key_list[1], 1), 0, BINS - 1).astype(jnp.int32),
        "absorb_bins": jnp.clip(jnp.exp(jax.random.uniform(key_list[2], (BINS,), jnp.float32, math.log(0.00234375), math.log(0.0625))), 0.00234375, 0.0625),
        "emit_bins": jnp.clip(jnp.exp(jax.random.uniform(key_list[3], (BINS,), jnp.float32, math.log(0.2), math.log(3.0))), 0.2, 3.0),
        "occupancy": set_ends((jax.random.randint(key_list[4], (N_DEPTH, N_ROWS, TILES), 0, 4) < 3).astype(jnp.int32), jax.random.fold_in(key_list[4], 1), 0, 1),
        "col_offsets": set_ends(jax.random.randint(key_list[5], (COLS,), 2, 7), jax.random.fold_in(key_list[5], 1), 2, 6).astype(jnp.int32),
        "row_offsets": set_ends(jax.random.randint(key_list[6], (ROWS_ALL,), 2, 7), jax.random.fold_in(key_list[6], 1), 2, 6).astype(jnp.int32),
    }


def resample_columns(mixed, col_offsets):
    fraction = col_offsets.astype(jnp.float32) / 8.0
    pad_shape = mixed.shape[:-1] + (1,)
    right_side = jnp.concatenate([mixed[..., 1:], jnp.zeros(pad_shape, jnp.float32)], -1)
    return (1.0 - fraction) * mixed + fraction * right_side


def tables(bin_of_level, absorb_bins, emit_bins):
    count_bins = absorb_bins.shape[0]
    onehot = (bin_of_level[:, None] == jnp.arange(count_bins, dtype=jnp.int32)[None, :]).astype(jnp.float32)
    return jnp.sum(onehot * absorb_bins[None, :], 1), jnp.sum(onehot * emit_bins[None, :], 1)


def classify(sampled, absorb_level, emit_level):
    levels = absorb_level.shape[0]
    scaled = sampled * float(levels - 1)
    absorption = jnp.zeros(sampled.shape, jnp.float32)
    emission = jnp.zeros(sampled.shape, jnp.float32)
    for knot_index in range(levels):
        weight = jnp.maximum(0.0, 1.0 - jnp.abs(scaled - float(knot_index)))
        absorption = absorption + weight * absorb_level[knot_index]
        emission = emission + weight * emit_level[knot_index]
    return absorption, emission


def composite(absorption, emission):
    inclusive = jnp.cumsum(absorption, 0)
    exclusive = inclusive - absorption
    light = jnp.sum(jnp.exp(-exclusive) * (1.0 - jnp.exp(-absorption)) * emission, 0)
    return light, inclusive[-1]


def reference(density, bin_of_level, absorb_bins, emit_bins, occupancy, col_offsets, row_offsets):
    absorb_level, emit_level = tables(bin_of_level, absorb_bins, emit_bins)
    frac_row = (row_offsets.astype(jnp.float32) / 8.0)[None, :, None]
    slabs = density.reshape(N_DEPTH, SLAB, ROWS_ALL, COLS)
    followers = jnp.concatenate([slabs[1:, 0], jnp.zeros((1, ROWS_ALL, COLS), jnp.float32)], 0)

    def per_slab(inputs):
        planes, following, occupied = inputs
        extended = jnp.concatenate([planes, following[None]], 0)
        mid_depth = 0.5 * (extended[:-1] + extended[1:])
        next_rows = jnp.concatenate([mid_depth[:, 1:], jnp.zeros((SLAB, 1, COLS), jnp.float32)], 1)
        mixed = (1.0 - frac_row) * mid_depth + frac_row * next_rows
        sampled = resample_columns(mixed, col_offsets)
        absorption, emission = classify(sampled, absorb_level, emit_level)
        brick_mask = jnp.repeat(jnp.repeat(occupied.astype(jnp.float32), ROW_DEV, 0), 128, 1)
        absorption = absorption * brick_mask[None]
        return composite(absorption, emission)

    lights, depths = lax.map(per_slab, (slabs, followers, occupancy))
    front_depth = jnp.cumsum(depths, 0) - depths
    front = jnp.exp(-front_depth)
    radiance = jnp.sum(front * lights, 0)
    remaining = jnp.exp(-jnp.sum(depths, 0))
    return front, jnp.stack([radiance, remaining])
```

```python
import functools
import math

import jax
import jax.numpy as jnp
from jax import lax
from jax.experimental import pallas as pl
from jax.experimental.pallas import tpu as pltpu
from jax.sharding import PartitionSpec as P

LANES = 128
SUB = 8
HALVES = 2
MESH = pl.DeviceIdType.MESH


def repeat(count, body):
    if count <= 16:
        for i in range(count):
            body(i)
    else:
        lax.fori_loop(0, count, lambda i, c: (body(i), c)[1], 0)


def pick(table, index):
    dims = lax.GatherDimensionNumbers(
        offset_dims=(),
        collapsed_slice_dims=(0,),
        start_index_map=(0,),
        operand_batching_dims=(1,),
        start_indices_batching_dims=(1,),
    )
    return lax.gather(
        table, index[..., None], dims, slice_sizes=(1, 1), mode=lax.GatherScatterMode.PROMISE_IN_BOUNDS
    )


def both(*conditions):
    return functools.reduce(jnp.logical_and, conditions)


def kernel(
    n_depth,
    n_rows,
    hosts,
    owners,
    dens_hbm,
    bins_hbm,
    absorb_hbm,
    emit_hbm,
    occ_hbm,
    col_hbm,
    row_hbm,
    front_ref,
    image_ref,
    dens,
    bins_ref,
    absorb_ref,
    emit_ref,
    occ_ref,
    col_ref,
    row_ref,
    row_send,
    row_halo,
    corner_send,
    corner,
    edge,
    state,
    parts,
    gathered,
    factors,
    pairs,
    factor_in,
    pair_in,
    load_sem,
    small_sem,
    depth_send_sem,
    depth_recv_sem,
    rows_send_sem,
    rows_recv_sem,
    corner_sem,
    part_send_sem,
    part_recv_sem,
    factor_send_sem,
    factor_recv_sem,
    pair_send_sem,
    pair_recv_sem,
):
    slab, rows, cols = dens_hbm.shape
    tiles = cols // LANES
    row_tiles = rows // SUB
    levels = bins_ref.shape[0]
    members = n_depth // HALVES
    per_owner = tiles // owners
    d = lax.axis_index("depth")
    r = lax.axis_index("rows")
    half = d // members
    m = lax.rem(d, members)
    slot = lax.rem(r, hosts)
    host_row = r - slot + hosts - 1
    is_host = slot == hosts - 1
    is_owner = both(is_host, m < owners)

    def load(c):
        return pltpu.make_async_copy(
            dens_hbm.at[:, :, c * LANES : (c + 1) * LANES],
            dens.at[c, pl.ds(0, slab), pl.ds(0, rows), :],
            load_sem.at[c],
        )

    small = [
        pltpu.make_async_copy(src, dst, small_sem.at[i])
        for i, (src, dst) in enumerate(
            (
                (bins_hbm, bins_ref),
                (absorb_hbm, absorb_ref),
                (emit_hbm, emit_ref),
                (occ_hbm, occ_ref),
                (col_hbm, col_ref),
                (row_hbm, row_ref),
            )
        )
    ]
    order = list(range(tiles - 1, -1, -1))
    for c in order:
        load(c).start()
    for copy in small:
        copy.start()

    barrier = pltpu.get_barrier_semaphore()

    def greet(dd, rr):
        pl.semaphore_signal(barrier, inc=1, device_id=(dd, rr), device_id_type=MESH)

    up_d, down_d = d > 0, d < n_depth - 1
    up_r, down_r = r > 0, r < n_rows - 1
    beside = (
        (up_d, d - 1, r),
        (up_r, d, r - 1),
        (both(up_d, up_r), d - 1, r - 1),
        (down_d, d + 1, r),
        (down_r, d, r + 1),
        (both(down_d, down_r), d + 1, r + 1),
    )
    expected = jnp.where(is_owner, n_depth * hosts - 1, HALVES * owners)
    for there, dd, rr in beside:
        pl.when(there)(functools.partial(greet, dd, rr))
        expected = expected + there.astype(jnp.int32)

    for s in range(hosts):

        def greet_block(j, s=s):
            wanted = is_owner
            if s == hosts - 1:
                wanted = jnp.logical_or(wanted, lax.rem(j, members) < owners)
            itself = both(j == d, slot == s)
            pl.when(both(wanted, jnp.logical_not(itself)))(
                functools.partial(greet, jnp.int32(j), host_row - hosts + 1 + s)
            )

        repeat(n_depth, greet_block)

    @pl.when(jnp.logical_not(down_d))
    def _():
        dens[:, slab] = jnp.zeros((tiles,) + dens.shape[2:], jnp.float32)

    lane = lax.broadcasted_iota(jnp.int32, (SUB, LANES), 1)
    sub = lax.broadcasted_iota(jnp.int32, (SUB, LANES), 0)
    last_lane = lane == LANES - 1

    for copy in small:
        copy.wait()

    def tables(values):
        values = values + values[-1:]
        out = []
        for first in range(0, levels, SUB):
            base = jnp.zeros((SUB, LANES), jnp.float32)
            slope = jnp.zeros((SUB, LANES), jnp.float32)
            for k in range(first, min(first + SUB, levels)):
                step = values[k + 1] - values[k]
                base = jnp.where(sub == k - first, values[k] - step * float(k), base)
                slope = jnp.where(sub == k - first, step, slope)
            out.append((base, slope))
        return out

    to_log2 = -math.log2(math.e)
    absorb = tables([absorb_ref[bins_ref[k]] * to_log2 for k in range(levels)])
    emit = tables([emit_ref[bins_ref[k]] for k in range(levels)])

    def absorb_of(c):
        occupied = occ_ref[0, 0, (c * LANES) // (cols // occ_ref.shape[2])].astype(jnp.float32)
        return [(base * occupied, slope * occupied) for base, slope in absorb]

    row_frac = []
    for t in range(row_tiles):
        frac = jnp.zeros((SUB, LANES), jnp.float32)
        for y in range(SUB):
            frac = jnp.where(sub == y, row_ref[t * SUB + y].astype(jnp.float32), frac)
        row_frac.append(frac / 8.0)

    def row_weights(t):
        if isinstance(t, int):
            frac = row_frac[t]
        else:
            frac = row_frac[-1]
            for i in range(row_tiles - 1):
                frac = jnp.where(t == i, row_frac[i], frac)
        gain = 0.5 * float(levels - 1)
        return gain * (1.0 - frac), gain * frac

    def col_weights(c):
        frac = jnp.broadcast_to(col_ref[c : c + 1, :].astype(jnp.float32) / 8.0, (SUB, LANES))
        keep = 1.0 - frac
        if c == tiles - 1:
            frac = jnp.where(last_lane, 0.0, frac)
        return keep, frac

    def rows_mixed(c, z, at, rw):
        return rw[0] * dens[c, z, pl.ds(at, SUB), :] + rw[1] * dens[c, z, pl.ds(at + 1, SUB), :]

    def cols_mixed(mixed, right_edge, cw):
        turned = pltpu.roll(mixed, LANES - 1, 1)
        return cw[0] * mixed + cw[1] * jnp.where(last_lane, right_edge, turned), turned

    def shade(prev, now, carry, absorb_c):
        through, depth, light = carry
        scaled = prev + now
        knot = lax.round(scaled - 0.5, lax.RoundingMethod.TO_NEAREST_EVEN).astype(jnp.int32)
        low = jnp.bitwise_and(knot, SUB - 1)

        def value(table):
            picked = [(pick(base, low), pick(slope, low)) for base, slope in table]
            base, slope = picked[-1]
            for i in range(len(picked) - 2, -1, -1):
                here = knot < (i + 1) * SUB
                base = jnp.where(here, picked[i][0], base)
                slope = jnp.where(here, picked[i][1], slope)
            return base + slope * scaled

        depth = depth + value(absorb_c)
        after = jnp.exp2(depth)
        light = light + (through - after) * value(emit)
        return after, depth, light

    zero = jnp.zeros((SUB, LANES), jnp.float32)
    one = jnp.ones((SUB, LANES), jnp.float32)

    def march(t):
        at = t * SUB
        if not isinstance(t, int):
            at = pl.multiple_of(at, SUB)
        rw = row_weights(t)
        for z in range(slab):
            edge[z] = zero
        for c in order:
            cw = col_weights(c)
            absorb_c = absorb_of(c)
            carry = (one, zero, zero)
            prev = None
            for z in range(slab):
                now, turned = cols_mixed(rows_mixed(c, z, at, rw), edge[z], cw)
                edge[z] = turned
                if prev is not None:
                    carry = shade(prev, now, carry, absorb_c)
                prev = now
            state[t, c, 0] = prev
            state[t, c, 1] = carry[1]
            state[t, c, 2] = carry[2]

    for c in order:
        load(c).wait()
        for z in range(slab):
            row_send[c, z : z + 1, :] = dens[c, z, 0:1, :]
        corner_send[c : c + 1, :] = dens[c, 0, 0:1, :]

    pl.semaphore_wait(barrier, expected)

    def remote(src, dst, send_sem, recv_sem, device):
        return pltpu.make_async_remote_copy(
            src_ref=src,
            dst_ref=dst,
            send_sem=send_sem,
            recv_sem=recv_sem,
            device_id=device,
            device_id_type=MESH,
        )

    def depth_copy(c):
        return remote(
            dens.at[c, 0, pl.ds(0, rows), :],
            dens.at[c, slab, pl.ds(0, rows), :],
            depth_send_sem.at[c],
            depth_recv_sem.at[c],
            (d - 1, r),
        )

    def rows_copy(c):
        return remote(row_send.at[c], row_halo.at[c], rows_send_sem.at[c], rows_recv_sem.at[c], (d, r - 1))

    corner_copy = remote(corner_send, corner, corner_sem.at[0], corner_sem.at[1], (d - 1, r - 1))

    @pl.when(up_d)
    def _():
        for c in order:
            depth_copy(c).start()

    @pl.when(up_r)
    def _():
        for c in order:
            rows_copy(c).start()

    pl.when(both(up_d, up_r))(corner_copy.start)

    for t in range(row_tiles):
        if t == row_tiles - 1:

            @pl.when(down_r)
            def _():
                for c in order:
                    rows_copy(c).wait_recv()
                    for z in range(slab):
                        dens[c, z, rows : rows + 1, :] = row_halo[c, z : z + 1, :]

            @pl.when(jnp.logical_not(down_r))
            def _():
                for c in order:
                    for z in range(slab):
                        dens[c, z, rows : rows + 1, :] = jnp.zeros((1, LANES), jnp.float32)

        march(t)

    @pl.when(both(down_d, down_r))
    def _():
        corner_copy.wait_recv()
        for c in order:
            dens[c, slab, rows : rows + 1, :] = corner[c : c + 1, :]

    @pl.when(both(down_d, jnp.logical_not(down_r)))
    def _():
        for c in order:
            dens[c, slab, rows : rows + 1, :] = jnp.zeros((1, LANES), jnp.float32)

    def owner_of(c):
        return lax.rem(c, owners), c // owners

    def part_copy(c, source, to_slot):
        q, k = owner_of(c)
        return remote(
            parts.at[c],
            gathered.at[to_slot, k, source],
            part_send_sem.at[c],
            part_recv_sem.at[to_slot, k, source],
            (half * members + q, host_row),
        )

    def own_tile(c):
        return both(is_host, m == owner_of(c)[0])

    edges = [zero] * row_tiles
    for c in order:
        pl.when(down_d)(depth_copy(c).wait_recv)
        cw = col_weights(c)
        absorb_c = absorb_of(c)
        for t in range(row_tiles):
            now, edges[t] = cols_mixed(rows_mixed(c, slab, t * SUB, row_weights(t)), edges[t], cw)
            depth = state[t, c, 1]
            carry = (jnp.exp2(depth), depth, state[t, c, 2])
            _, depth, light = shade(state[t, c, 0], now, carry, absorb_c)
            parts[c, 0, t * SUB : (t + 1) * SUB, :] = depth
            parts[c, 1, t * SUB : (t + 1) * SUB, :] = light

        @pl.when(jnp.logical_not(own_tile(c)))
        def _():
            part_copy(c, m, slot).start()

        @pl.when(own_tile(c))
        def _():
            gathered[hosts - 1, c // owners, pl.ds(m, 1)] = parts[pl.ds(c, 1)]

    def pair_copy(s, k, target, from_half, c):
        return remote(
            pairs.at[s, k],
            pair_in.at[from_half, c],
            pair_send_sem.at[s, k, target],
            pair_recv_sem.at[from_half, c],
            (target, host_row - hosts + 1 + s),
        )

    def factor_copy(s, k, j, c):
        return remote(
            factors.at[s, k, j],
            factor_in.at[c],
            factor_send_sem.at[s, k, j],
            factor_recv_sem.at[c],
            (half * members + j, host_row - hosts + 1 + s),
        )

    def elsewhere(s, j, body):
        if s == hosts - 1:
            pl.when(j != d)(body)
        else:
            body()

    def compose(k, s):
        mine = k * owners + m

        def arrived(j):
            elsewhere(
                s,
                half * members + j,
                lambda: remote(
                    parts.at[mine],
                    gathered.at[s, k, j],
                    part_send_sem.at[mine],
                    part_recv_sem.at[s, k, j],
                    (half * members + j, host_row),
                ).wait_recv(),
            )

        repeat(members, arrived)

        def add(j, carry):
            total, radiance = carry
            factor = jnp.exp2(total)
            factors[s, k, j] = factor
            return total + gathered[s, k, j, 0], radiance + factor * gathered[s, k, j, 1]

        blank = jnp.zeros((rows, LANES), jnp.float32)
        carry = (blank, blank)
        if members <= 16:
            for j in range(members):
                carry = add(j, carry)
        else:
            carry = lax.fori_loop(0, members, add, carry)
        pairs[s, k, 0] = carry[0]
        pairs[s, k, 1] = carry[1]

        def reply(target):
            elsewhere(s, target, lambda: pair_copy(s, k, target, half, mine).start())

        def reply_own(j):
            elsewhere(s, half * members + j, lambda: factor_copy(s, k, j, mine).start())

        repeat(n_depth, reply)
        repeat(members, reply_own)
        if s == hosts - 1:
            pair_in[half, mine] = pairs[s, k]
            factor_in[mine] = factors[s, k, m]

    @pl.when(is_owner)
    def _():
        for k in range(per_owner - 1, -1, -1):
            for s in range(hosts):
                compose(k, s)

    def from_other(c, h, body):
        q, _ = owner_of(c)
        pl.when(jnp.logical_not(both(is_host, d == h * members + q)))(body)

    for c in order:
        for h in range(HALVES):
            from_other(c, h, pair_copy(0, 0, d, h, c).wait_recv)
        pl.when(jnp.logical_not(own_tile(c)))(factor_copy(0, 0, m, c).wait_recv)
        where = slice(c * LANES, (c + 1) * LANES)
        before = jnp.exp2(pair_in[0, c, 0])
        ahead = jnp.where(half > 0, before, 1.0)
        front_ref[0, :, where] = ahead * factor_in[c]
        image_ref[0, :, where] = pair_in[0, c, 1] + before * pair_in[1, c, 1]
        image_ref[1, :, where] = before * jnp.exp2(pair_in[1, c, 0])

    @pl.when(up_d)
    def _():
        for c in order:
            depth_copy(c).wait_send()

    @pl.when(up_r)
    def _():
        for c in order:
            rows_copy(c).wait_send()

    pl.when(both(up_d, up_r))(corner_copy.wait_send)
    for c in order:
        pl.when(jnp.logical_not(own_tile(c)))(part_copy(c, m, slot).wait_send)

    @pl.when(is_owner)
    def _():
        for k in range(per_owner):
            for s in range(hosts):
                repeat(n_depth, lambda j: elsewhere(s, j, pair_copy(s, k, j, half, k * owners + m).wait_send))
                repeat(
                    members,
                    lambda j: elsewhere(s, half * members + j, factor_copy(s, k, j, k * owners + m).wait_send),
                )


def on_device(n_depth, n_rows, density, bin_of_level, absorb_bins, emit_bins, occupancy, col_offsets, row_offsets):
    slab, rows, cols = density.shape
    tiles = cols // LANES
    row_tiles = rows // SUB
    members = n_depth // HALVES
    hosts = 2 if n_rows % 2 == 0 else 1
    owners = 1
    while owners * 2 <= members and tiles % (owners * 2) == 0:
        owners *= 2
    per_owner = tiles // owners
    anywhere = pl.BlockSpec(memory_space=pl.ANY)
    vmem = pl.BlockSpec(memory_space=pltpu.VMEM)
    f32, i32 = jnp.float32, jnp.int32
    dma = pltpu.SemaphoreType.DMA
    return pl.pallas_call(
        functools.partial(kernel, n_depth, n_rows, hosts, owners),
        out_shape=(pltpu.VMEM((1, rows, cols), f32), pltpu.VMEM((2, rows, cols), f32)),
        in_specs=[anywhere] * 7,
        out_specs=(vmem, vmem),
        scratch_shapes=[
            pltpu.VMEM((tiles, slab + 1, rows + SUB, LANES), f32),
            pltpu.SMEM(bin_of_level.shape, i32),
            pltpu.SMEM(absorb_bins.shape, f32),
            pltpu.SMEM(emit_bins.shape, f32),
            pltpu.SMEM(occupancy.shape, i32),
            pltpu.VMEM((tiles, LANES), i32),
            pltpu.SMEM(row_offsets.shape, i32),
            pltpu.VMEM((tiles, slab, LANES), f32),
            pltpu.VMEM((tiles, slab, LANES), f32),
            pltpu.VMEM((tiles, LANES), f32),
            pltpu.VMEM((tiles, LANES), f32),
            pltpu.VMEM((slab, SUB, LANES), f32),
            pltpu.VMEM((row_tiles, tiles, 3, SUB, LANES), f32),
            pltpu.VMEM((tiles, 2, rows, LANES), f32),
            pltpu.VMEM((hosts, per_owner, members, 2, rows, LANES), f32),
            pltpu.VMEM((hosts, per_owner, members, rows, LANES), f32),
            pltpu.VMEM((hosts, per_owner, 2, rows, LANES), f32),
            pltpu.VMEM((tiles, rows, LANES), f32),
            pltpu.VMEM((HALVES, tiles, 2, rows, LANES), f32),
            dma((tiles,)),
            dma((6,)),
            dma((tiles,)),
            dma((tiles,)),
            dma((tiles,)),
            dma((tiles,)),
            dma((2,)),
            dma((tiles,)),
            dma((hosts, per_owner, members)),
            dma((hosts, per_owner, members)),
            dma((tiles,)),
            dma((hosts, per_owner, n_depth)),
            dma((HALVES, tiles)),
        ],
        compiler_params=pltpu.CompilerParams(collective_id=0, has_side_effects=True),
    )(
        density,
        bin_of_level,
        absorb_bins,
        emit_bins,
        occupancy,
        col_offsets.reshape(tiles, LANES),
        row_offsets,
    )


def solution(mesh):
    placed = (P("depth", "rows", None), P(), P(), P(), P("depth", "rows", None), P(), P("rows"))
    return jax.shard_map(
        functools.partial(on_device, mesh.shape["depth"], mesh.shape["rows"]),
        mesh=mesh,
        in_specs=placed,
        out_specs=(P("depth", "rows", None), P(None, "rows", None)),
        check_vma=False,
    )
```

```python
import functools
import math

import jax
import jax.numpy as jnp
from jax import lax
from jax.experimental import pallas as pl
from jax.experimental.pallas import tpu as pltpu
from jax.sharding import PartitionSpec as P

LANES = 128
SUB = 8
HALVES = 2
MESH = pl.DeviceIdType.MESH


def repeat(count, body):
    if count <= 16:
        for i in range(count):
            body(i)
    else:
        lax.fori_loop(0, count, lambda i, c: (body(i), c)[1], 0)


def pick(table, index):
    dims = lax.GatherDimensionNumbers(
        offset_dims=(),
        collapsed_slice_dims=(0,),
        start_index_map=(0,),
        operand_batching_dims=(1,),
        start_indices_batching_dims=(1,),
    )
    return lax.gather(
        table, index[..., None], dims, slice_sizes=(1, 1), mode=lax.GatherScatterMode.PROMISE_IN_BOUNDS
    )


def both(*conditions):
    return functools.reduce(jnp.logical_and, conditions)


def kernel(
    n_depth,
    n_rows,
    hosts,
    owners,
    dens_hbm,
    bins_hbm,
    absorb_hbm,
    emit_hbm,
    occ_hbm,
    col_hbm,
    row_hbm,
    front_ref,
    image_ref,
    dens,
    bins_ref,
    absorb_ref,
    emit_ref,
    occ_ref,
    col_ref,
    row_ref,
    row_send,
    row_halo,
    corner_send,
    corner,
    edge,
    state,
    parts,
    gathered,
    factors,
    pairs,
    factor_in,
    pair_in,
    first_sem,
    rows_sem,
    load_sem,
    small_sem,
    ready,
    depth_send_sem,
    depth_recv_sem,
    rows_send_sem,
    rows_recv_sem,
    corner_sem,
    part_send_sem,
    part_recv_sem,
    factor_send_sem,
    factor_recv_sem,
    pair_send_sem,
    pair_recv_sem,
):
    slab, rows, cols = dens_hbm.shape
    tiles = cols // LANES
    row_tiles = rows // SUB
    levels = bins_ref.shape[0]
    members = n_depth // HALVES
    per_owner = tiles // owners
    d = lax.axis_index("depth")
    r = lax.axis_index("rows")
    half = d // members
    m = lax.rem(d, members)
    slot = lax.rem(r, hosts)
    host_row = r - slot + hosts - 1
    is_host = slot == hosts - 1
    is_owner = both(is_host, m < owners)

    def first_load(c):
        return pltpu.make_async_copy(
            dens_hbm.at[0, :, pl.ds(c * LANES, LANES)],
            dens.at[c, 0, pl.ds(0, rows), :],
            first_sem.at[c],
        )

    def rows_load(c):
        return pltpu.make_async_copy(
            dens_hbm.at[:, 0, pl.ds(c * LANES, LANES)],
            row_send.at[c],
            rows_sem.at[c],
        )

    def load(c):
        return pltpu.make_async_copy(
            dens_hbm.at[pl.ds(1, slab - 1), :, pl.ds(c * LANES, LANES)],
            dens.at[c, pl.ds(1, slab - 1), pl.ds(0, rows), :],
            load_sem.at[c],
        )

    small = [
        pltpu.make_async_copy(src, dst, small_sem.at[i])
        for i, (src, dst) in enumerate(
            (
                (bins_hbm, bins_ref),
                (absorb_hbm, absorb_ref),
                (emit_hbm, emit_ref),
                (occ_hbm, occ_ref),
                (col_hbm, col_ref),
                (row_hbm, row_ref),
            )
        )
    ]
    barrier = pltpu.get_barrier_semaphore()
    up_d, down_d = d > 0, d < n_depth - 1
    up_r, down_r = r > 0, r < n_rows - 1

    def greet(semaphore, dd, rr):
        pl.semaphore_signal(semaphore, inc=1, device_id=(dd, rr), device_id_type=MESH)

    for there, dd, rr in ((down_d, d + 1, r), (down_r, d, r + 1), (both(down_d, down_r), d + 1, r + 1)):
        pl.when(there)(functools.partial(greet, barrier, dd, rr))

    order = list(range(tiles - 1, -1, -1))
    for c in order:
        first_load(c).start()
    for c in order:
        rows_load(c).start()
    for c in order:
        load(c).start()
    for copy in small:
        copy.start()

    def greet_block(semaphore, later):
        for s in range(hosts):

            def one(j, s=s):
                wanted = is_owner
                if s == hosts - 1:
                    wanted = jnp.logical_or(wanted, lax.rem(j, members) < owners)
                if later:
                    side = jnp.logical_or(j > d, both(j == d, s > slot))
                else:
                    side = jnp.logical_or(j < d, both(j == d, s < slot))
                pl.when(both(wanted, side))(
                    functools.partial(greet, semaphore, jnp.int32(j), host_row - hosts + 1 + s)
                )

            repeat(n_depth, one)

    greet_block(barrier, True)
    earlier = jnp.where(is_owner, d * hosts + slot, half * owners + jnp.minimum(m, owners))
    related = jnp.where(is_owner, n_depth * hosts - 1, HALVES * owners)
    expected = earlier
    for there in (up_d, up_r, both(up_d, up_r)):
        expected = expected + there.astype(jnp.int32)

    def remote(src, dst, send_sem, recv_sem, device):
        return pltpu.make_async_remote_copy(
            src_ref=src,
            dst_ref=dst,
            send_sem=send_sem,
            recv_sem=recv_sem,
            device_id=device,
            device_id_type=MESH,
        )

    def depth_copy(c):
        return remote(
            dens.at[c, 0, pl.ds(0, rows), :],
            dens.at[c, slab, pl.ds(0, rows), :],
            depth_send_sem.at[c],
            depth_recv_sem.at[c],
            (d - 1, r),
        )

    def rows_copy(c):
        return remote(row_send.at[c], row_halo.at[c], rows_send_sem.at[c], rows_recv_sem.at[c], (d, r - 1))

    corner_copy = remote(corner_send, corner, corner_sem.at[0], corner_sem.at[1], (d - 1, r - 1))

    pl.when(expected > 0)(lambda: pl.semaphore_wait(barrier, expected))
    for c in order:
        first_load(c).wait()
        pl.when(up_d)(depth_copy(c).start)
    for c in order:
        rows_load(c).wait()
        corner_send[c : c + 1, :] = row_send[c, 0:1, :]
        pl.when(up_r)(rows_copy(c).start)
    greet_block(ready, False)
    pl.when(both(up_d, up_r))(corner_copy.start)

    @pl.when(jnp.logical_not(down_d))
    def _():
        dens[:, slab] = jnp.zeros((tiles,) + dens.shape[2:], jnp.float32)

    lane = lax.broadcasted_iota(jnp.int32, (SUB, LANES), 1)
    sub = lax.broadcasted_iota(jnp.int32, (SUB, LANES), 0)
    last_lane = lane == LANES - 1

    for copy in small:
        copy.wait()

    def tables(values):
        values = values + values[-1:]
        out = []
        for first in range(0, levels, SUB):
            base = jnp.zeros((SUB, LANES), jnp.float32)
            slope = jnp.zeros((SUB, LANES), jnp.float32)
            for k in range(first, min(first + SUB, levels)):
                step = values[k + 1] - values[k]
                base = jnp.where(sub == k - first, values[k] - step * float(k), base)
                slope = jnp.where(sub == k - first, step, slope)
            out.append((base, slope))
        return out

    to_log2 = -math.log2(math.e)
    absorb = tables([absorb_ref[bins_ref[k]] * to_log2 for k in range(levels)])
    emit = tables([emit_ref[bins_ref[k]] for k in range(levels)])

    def absorb_of(c):
        occupied = occ_ref[0, 0, (c * LANES) // (cols // occ_ref.shape[2])].astype(jnp.float32)
        return [(base * occupied, slope * occupied) for base, slope in absorb]

    row_frac = []
    for t in range(row_tiles):
        frac = jnp.zeros((SUB, LANES), jnp.float32)
        for y in range(SUB):
            frac = jnp.where(sub == y, row_ref[t * SUB + y].astype(jnp.float32), frac)
        row_frac.append(frac / 8.0)

    def row_weights(t):
        if isinstance(t, int):
            frac = row_frac[t]
        else:
            frac = row_frac[-1]
            for i in range(row_tiles - 1):
                frac = jnp.where(t == i, row_frac[i], frac)
        gain = 0.5 * float(levels - 1)
        return gain * (1.0 - frac), gain * frac

    def col_weights(c):
        frac = jnp.broadcast_to(col_ref[c : c + 1, :].astype(jnp.float32) / 8.0, (SUB, LANES))
        keep = 1.0 - frac
        if c == tiles - 1:
            frac = jnp.where(last_lane, 0.0, frac)
        return keep, frac

    def rows_mixed(c, z, at, rw):
        return rw[0] * dens[c, z, pl.ds(at, SUB), :] + rw[1] * dens[c, z, pl.ds(at + 1, SUB), :]

    def cols_mixed(mixed, right_edge, cw):
        turned = pltpu.roll(mixed, LANES - 1, 1)
        return cw[0] * mixed + cw[1] * jnp.where(last_lane, right_edge, turned), turned

    def shade(prev, now, carry, absorb_c):
        through, depth, light = carry
        scaled = prev + now
        knot = lax.round(scaled - 0.5, lax.RoundingMethod.TO_NEAREST_EVEN).astype(jnp.int32)
        low = jnp.bitwise_and(knot, SUB - 1)

        def value(table):
            picked = [(pick(base, low), pick(slope, low)) for base, slope in table]
            base, slope = picked[-1]
            for i in range(len(picked) - 2, -1, -1):
                here = knot < (i + 1) * SUB
                base = jnp.where(here, picked[i][0], base)
                slope = jnp.where(here, picked[i][1], slope)
            return base + slope * scaled

        depth = depth + value(absorb_c)
        after = jnp.exp2(depth)
        light = light + (through - after) * value(emit)
        return after, depth, light

    zero = jnp.zeros((SUB, LANES), jnp.float32)
    one = jnp.ones((SUB, LANES), jnp.float32)

    def march(t):
        at = t * SUB
        if not isinstance(t, int):
            at = pl.multiple_of(at, SUB)
        rw = row_weights(t)
        for z in range(slab):
            edge[z] = zero
        for n, c in enumerate(order):
            if t == row_tiles - 1 and n % 4 == 0:
                fill_rows(order[n : n + 4])
            cw = col_weights(c)
            absorb_c = absorb_of(c)
            carry = (one, zero, zero)
            prev = None
            for z in range(slab):
                now, turned = cols_mixed(rows_mixed(c, z, at, rw), edge[z], cw)
                edge[z] = turned
                if prev is not None:
                    carry = shade(prev, now, carry, absorb_c)
                prev = now
            state[t, c, 0] = prev
            state[t, c, 1] = carry[1]
            state[t, c, 2] = carry[2]

    for c in order:
        load(c).wait()

    def fill_rows(group_tiles):
        @pl.when(down_r)
        def _():
            for c in group_tiles:
                rows_copy(c).wait_recv()
                for z in range(slab):
                    dens[c, z, rows : rows + 1, :] = row_halo[c, z : z + 1, :]

        @pl.when(jnp.logical_not(down_r))
        def _():
            for c in group_tiles:
                for z in range(slab):
                    dens[c, z, rows : rows + 1, :] = jnp.zeros((1, LANES), jnp.float32)

    for t in range(row_tiles):
        march(t)

    @pl.when(both(down_d, down_r))
    def _():
        corner_copy.wait_recv()
        for c in order:
            dens[c, slab, rows : rows + 1, :] = corner[c : c + 1, :]

    @pl.when(both(down_d, jnp.logical_not(down_r)))
    def _():
        for c in order:
            dens[c, slab, rows : rows + 1, :] = jnp.zeros((1, LANES), jnp.float32)

    def owner_of(c):
        return lax.rem(c, owners), c // owners

    def part_copy(c, source, to_slot):
        q, k = owner_of(c)
        return remote(
            parts.at[c],
            gathered.at[to_slot, k, source],
            part_send_sem.at[c],
            part_recv_sem.at[to_slot, k, source],
            (half * members + q, host_row),
        )

    def own_tile(c):
        return both(is_host, m == owner_of(c)[0])

    pl.when(related > earlier)(lambda: pl.semaphore_wait(ready, related - earlier))
    edges = [zero] * row_tiles
    for c in order:
        pl.when(down_d)(depth_copy(c).wait_recv)
        cw = col_weights(c)
        absorb_c = absorb_of(c)
        for t in range(row_tiles):
            now, edges[t] = cols_mixed(rows_mixed(c, slab, t * SUB, row_weights(t)), edges[t], cw)
            depth = state[t, c, 1]
            carry = (jnp.exp2(depth), depth, state[t, c, 2])
            _, depth, light = shade(state[t, c, 0], now, carry, absorb_c)
            parts[c, 0, t * SUB : (t + 1) * SUB, :] = depth
            parts[c, 1, t * SUB : (t + 1) * SUB, :] = light

        @pl.when(jnp.logical_not(own_tile(c)))
        def _():
            part_copy(c, m, slot).start()

        @pl.when(own_tile(c))
        def _():
            gathered[hosts - 1, c // owners, pl.ds(m, 1)] = parts[pl.ds(c, 1)]

    def pair_copy(s, target, from_half, q):
        return remote(
            pairs.at[s],
            pair_in.at[from_half, q],
            pair_send_sem.at[s, target],
            pair_recv_sem.at[from_half, q],
            (target, host_row - hosts + 1 + s),
        )

    def factor_copy(s, j, q):
        return remote(
            factors.at[s, j],
            factor_in.at[q],
            factor_send_sem.at[s, j],
            factor_recv_sem.at[q],
            (half * members + j, host_row - hosts + 1 + s),
        )

    def elsewhere(s, j, body):
        if s == hosts - 1:
            pl.when(j != d)(body)
        else:
            body()

    def compose(k, s):
        mine = k * owners + m

        def arrived(j):
            elsewhere(
                s,
                half * members + j,
                lambda: remote(
                    parts.at[mine],
                    gathered.at[s, k, j],
                    part_send_sem.at[mine],
                    part_recv_sem.at[s, k, j],
                    (half * members + j, host_row),
                ).wait_recv(),
            )

        repeat(members, arrived)

        def add(j, carry):
            total, radiance = carry
            factor = jnp.exp2(total)
            factors[s, j, k] = factor
            return total + gathered[s, k, j, 0], radiance + factor * gathered[s, k, j, 1]

        blank = jnp.zeros((rows, LANES), jnp.float32)
        carry = (blank, blank)
        if members <= 16:
            for j in range(members):
                carry = add(j, carry)
        else:
            carry = lax.fori_loop(0, members, add, carry)
        pairs[s, k, 0] = carry[0]
        pairs[s, k, 1] = carry[1]

        if s == hosts - 1:
            pair_in[half, m, k] = pairs[s, k]
            factor_in[m, k] = factors[s, m, k]

    rounds = [(k, s) for k in range(per_owner - 1, -1, -1) for s in range(hosts)]

    def reply(target):
        j = lax.rem(target, members)
        for s in range(hosts):
            pl.when(half == target // members)(lambda: elsewhere(s, target, factor_copy(s, j, m).start))
            elsewhere(s, target, pair_copy(s, target, half, m).start)

    @pl.when(is_owner)
    def _():
        for k, s in rounds:
            compose(k, s)
        repeat(n_depth, reply)

    for q in range(owners - 1, -1, -1):
        for h in range(HALVES):
            itself = both(is_host, d == h * members + q)
            pl.when(jnp.logical_not(itself))(pair_copy(0, d, h, q).wait_recv)
        pl.when(jnp.logical_not(both(is_host, m == q)))(factor_copy(0, m, q).wait_recv)
        for k in range(per_owner):
            c = k * owners + q
            where = slice(c * LANES, (c + 1) * LANES)
            before = jnp.exp2(pair_in[0, q, k, 0])
            ahead = jnp.where(half > 0, before, 1.0)
            front_ref[0, :, where] = ahead * factor_in[q, k]
            image_ref[0, :, where] = pair_in[0, q, k, 1] + before * pair_in[1, q, k, 1]
            image_ref[1, :, where] = before * jnp.exp2(pair_in[1, q, k, 0])

    @pl.when(up_d)
    def _():
        for c in order:
            depth_copy(c).wait_send()

    @pl.when(up_r)
    def _():
        for c in order:
            rows_copy(c).wait_send()

    pl.when(both(up_d, up_r))(corner_copy.wait_send)
    for c in order:
        pl.when(jnp.logical_not(own_tile(c)))(part_copy(c, m, slot).wait_send)

    @pl.when(is_owner)
    def _():
        for s in range(hosts):
            repeat(n_depth, lambda j: elsewhere(s, j, pair_copy(s, j, half, m).wait_send))
            repeat(members, lambda j: elsewhere(s, half * members + j, factor_copy(s, j, m).wait_send))


def on_device(n_depth, n_rows, density, bin_of_level, absorb_bins, emit_bins, occupancy, col_offsets, row_offsets):
    slab, rows, cols = density.shape
    tiles = cols // LANES
    row_tiles = rows // SUB
    members = n_depth // HALVES
    hosts = 2 if n_rows % 2 == 0 else 1
    owners = 1
    while owners * 2 <= members and tiles % (owners * 2) == 0:
        owners *= 2
    per_owner = tiles // owners
    anywhere = pl.BlockSpec(memory_space=pl.ANY)
    vmem = pl.BlockSpec(memory_space=pltpu.VMEM)
    f32, i32 = jnp.float32, jnp.int32
    dma = pltpu.SemaphoreType.DMA
    return pl.pallas_call(
        functools.partial(kernel, n_depth, n_rows, hosts, owners),
        out_shape=(pltpu.VMEM((1, rows, cols), f32), pltpu.VMEM((2, rows, cols), f32)),
        in_specs=[anywhere] * 7,
        out_specs=(vmem, vmem),
        scratch_shapes=[
            pltpu.VMEM((tiles, slab + 1, rows + SUB, LANES), f32),
            pltpu.SMEM(bin_of_level.shape, i32),
            pltpu.SMEM(absorb_bins.shape, f32),
            pltpu.SMEM(emit_bins.shape, f32),
            pltpu.SMEM(occupancy.shape, i32),
            pltpu.VMEM((tiles, LANES), i32),
            pltpu.SMEM(row_offsets.shape, i32),
            pltpu.VMEM((tiles, slab, LANES), f32),
            pltpu.VMEM((tiles, slab, LANES), f32),
            pltpu.VMEM((tiles, LANES), f32),
            pltpu.VMEM((tiles, LANES), f32),
            pltpu.VMEM((slab, SUB, LANES), f32),
            pltpu.VMEM((row_tiles, tiles, 3, SUB, LANES), f32),
            pltpu.VMEM((tiles, 2, rows, LANES), f32),
            pltpu.VMEM((hosts, per_owner, members, 2, rows, LANES), f32),
            pltpu.VMEM((hosts, members, per_owner, rows, LANES), f32),
            pltpu.VMEM((hosts, per_owner, 2, rows, LANES), f32),
            pltpu.VMEM((owners, per_owner, rows, LANES), f32),
            pltpu.VMEM((HALVES, owners, per_owner, 2, rows, LANES), f32),
            dma((tiles,)),
            dma((tiles,)),
            dma((tiles,)),
            dma((6,)),
            pltpu.SemaphoreType.REGULAR,
            dma((tiles,)),
            dma((tiles,)),
            dma((tiles,)),
            dma((tiles,)),
            dma((2,)),
            dma((tiles,)),
            dma((hosts, per_owner, members)),
            dma((hosts, members)),
            dma((owners,)),
            dma((hosts, n_depth)),
            dma((HALVES, owners)),
        ],
        compiler_params=pltpu.CompilerParams(collective_id=0, has_side_effects=True),
    )(
        density,
        bin_of_level,
        absorb_bins,
        emit_bins,
        occupancy,
        col_offsets.reshape(tiles, LANES),
        row_offsets,
    )


def solution(mesh):
    placed = (P("depth", "rows", None), P(), P(), P(), P("depth", "rows", None), P(), P("rows"))
    return jax.shard_map(
        functools.partial(on_device, mesh.shape["depth"], mesh.shape["rows"]),
        mesh=mesh,
        in_specs=placed,
        out_specs=(P("depth", "rows", None), P(None, "rows", None)),
        check_vma=False,
    )
```

```python
import functools
import math

import jax
import jax.numpy as jnp
from jax import lax
from jax.experimental import pallas as pl
from jax.experimental.pallas import tpu as pltpu
from jax.sharding import PartitionSpec as P

LANES = 128
SUB = 8
HALVES = 2
MESH = pl.DeviceIdType.MESH


def repeat(count, body):
    if count <= 16:
        for i in range(count):
            body(i)
    else:
        lax.fori_loop(0, count, lambda i, c: (body(i), c)[1], 0)


def pick(table, index):
    dims = lax.GatherDimensionNumbers(
        offset_dims=(),
        collapsed_slice_dims=(0,),
        start_index_map=(0,),
        operand_batching_dims=(1,),
        start_indices_batching_dims=(1,),
    )
    return lax.gather(
        table, index[..., None], dims, slice_sizes=(1, 1), mode=lax.GatherScatterMode.PROMISE_IN_BOUNDS
    )


def both(*conditions):
    return functools.reduce(jnp.logical_and, conditions)


def kernel(
    n_depth,
    n_rows,
    hosts,
    owners,
    dens_hbm,
    bins_hbm,
    absorb_hbm,
    emit_hbm,
    occ_hbm,
    col_hbm,
    row_hbm,
    front_ref,
    image_ref,
    dens,
    bins_ref,
    absorb_ref,
    emit_ref,
    occ_ref,
    col_ref,
    row_ref,
    row_send,
    row_halo,
    corner_send,
    corner,
    edge,
    state,
    parts,
    gathered,
    factors,
    pairs,
    factor_in,
    pair_in,
    first_sem,
    rows_sem,
    load_sem,
    small_sem,
    ready,
    depth_send_sem,
    depth_recv_sem,
    rows_send_sem,
    rows_recv_sem,
    corner_sem,
    part_send_sem,
    part_recv_sem,
    factor_send_sem,
    factor_recv_sem,
    pair_send_sem,
    pair_recv_sem,
):
    slab, rows, cols = dens_hbm.shape
    tiles = cols // LANES
    row_tiles = rows // SUB
    levels = bins_ref.shape[0]
    members = n_depth // HALVES
    per_owner = tiles // owners
    d = lax.axis_index("depth")
    r = lax.axis_index("rows")
    half = d // members
    m = lax.rem(d, members)
    slot = lax.rem(r, hosts)
    host_row = r - slot + hosts - 1
    is_host = slot == hosts - 1
    is_owner = both(is_host, m < owners)

    def first_load(c):
        return pltpu.make_async_copy(
            dens_hbm.at[0, :, pl.ds(c * LANES, LANES)],
            dens.at[c, 0, pl.ds(0, rows), :],
            first_sem,
        )

    def rows_load(c):
        return pltpu.make_async_copy(
            dens_hbm.at[:, 0, pl.ds(c * LANES, LANES)],
            row_send.at[c],
            rows_sem,
        )

    def load(c):
        return pltpu.make_async_copy(
            dens_hbm.at[pl.ds(1, slab - 1), :, pl.ds(c * LANES, LANES)],
            dens.at[c, pl.ds(1, slab - 1), pl.ds(0, rows), :],
            load_sem,
        )

    small = [
        pltpu.make_async_copy(src, dst, small_sem.at[i])
        for i, (src, dst) in enumerate(
            (
                (bins_hbm, bins_ref),
                (absorb_hbm, absorb_ref),
                (emit_hbm, emit_ref),
                (occ_hbm, occ_ref),
                (col_hbm, col_ref),
                (row_hbm, row_ref),
            )
        )
    ]
    def landed(ref, semaphore):
        pltpu.make_async_copy(ref, ref, semaphore).wait()

    barrier = pltpu.get_barrier_semaphore()
    up_d, down_d = d > 0, d < n_depth - 1
    up_r, down_r = r > 0, r < n_rows - 1

    def greet(semaphore, dd, rr):
        pl.semaphore_signal(semaphore, inc=1, device_id=(dd, rr), device_id_type=MESH)

    for there, dd, rr in ((down_d, d + 1, r), (down_r, d, r + 1), (both(down_d, down_r), d + 1, r + 1)):
        pl.when(there)(functools.partial(greet, barrier, dd, rr))

    group = 4 if tiles % 4 == 0 else 1
    order = list(range(tiles - 1, -1, -1))
    for c in order:
        first_load(c).start()
    for c in order:
        rows_load(c).start()
    for c in order:
        load(c).start()
    for copy in small:
        copy.start()

    def greet_block(semaphore, later):
        for s in range(hosts):

            def one(j, s=s):
                wanted = is_owner
                if s == hosts - 1:
                    wanted = jnp.logical_or(wanted, lax.rem(j, members) < owners)
                if later:
                    side = jnp.logical_or(j > d, both(j == d, s > slot))
                else:
                    side = jnp.logical_or(j < d, both(j == d, s < slot))
                pl.when(both(wanted, side))(
                    functools.partial(greet, semaphore, jnp.int32(j), host_row - hosts + 1 + s)
                )

            repeat(n_depth, one)

    greet_block(barrier, True)
    earlier = jnp.where(is_owner, d * hosts + slot, half * owners + jnp.minimum(m, owners))
    related = jnp.where(is_owner, n_depth * hosts - 1, HALVES * owners)
    expected = earlier
    for there in (up_d, up_r, both(up_d, up_r)):
        expected = expected + there.astype(jnp.int32)

    def remote(src, dst, send_sem, recv_sem, device):
        return pltpu.make_async_remote_copy(
            src_ref=src,
            dst_ref=dst,
            send_sem=send_sem,
            recv_sem=recv_sem,
            device_id=device,
            device_id_type=MESH,
        )

    def depth_copy(c):
        return remote(
            dens.at[c, 0, pl.ds(0, rows), :],
            dens.at[c, slab, pl.ds(0, rows), :],
            depth_send_sem,
            depth_recv_sem.at[c // group],
            (d - 1, r),
        )

    def rows_copy(c):
        return remote(row_send.at[c], row_halo.at[c], rows_send_sem, rows_recv_sem.at[c // group], (d, r - 1))

    corner_copy = remote(corner_send, corner, corner_sem.at[0], corner_sem.at[1], (d - 1, r - 1))

    pl.when(expected > 0)(lambda: pl.semaphore_wait(barrier, expected))
    landed(dens.at[:, 0, pl.ds(0, rows), :], first_sem)

    @pl.when(up_d)
    def _():
        for c in order:
            depth_copy(c).start()

    landed(row_send, rows_sem)
    for c in order:
        corner_send[c : c + 1, :] = row_send[c, 0:1, :]

    @pl.when(up_r)
    def _():
        for c in order:
            rows_copy(c).start()

    greet_block(ready, False)
    pl.when(both(up_d, up_r))(corner_copy.start)

    @pl.when(jnp.logical_not(down_d))
    def _():
        dens[:, slab] = jnp.zeros((tiles,) + dens.shape[2:], jnp.float32)

    lane = lax.broadcasted_iota(jnp.int32, (SUB, LANES), 1)
    sub = lax.broadcasted_iota(jnp.int32, (SUB, LANES), 0)
    last_lane = lane == LANES - 1

    for copy in small:
        copy.wait()

    def tables(values):
        values = values + values[-1:]
        out = []
        for first in range(0, levels, SUB):
            base = jnp.zeros((SUB, LANES), jnp.float32)
            slope = jnp.zeros((SUB, LANES), jnp.float32)
            for k in range(first, min(first + SUB, levels)):
                step = values[k + 1] - values[k]
                base = jnp.where(sub == k - first, values[k] - step * float(k), base)
                slope = jnp.where(sub == k - first, step, slope)
            out.append((base, slope))
        return out

    to_log2 = -math.log2(math.e)
    absorb = tables([absorb_ref[bins_ref[k]] * to_log2 for k in range(levels)])
    emit = tables([emit_ref[bins_ref[k]] for k in range(levels)])

    def absorb_of(c):
        occupied = occ_ref[0, 0, (c * LANES) // (cols // occ_ref.shape[2])].astype(jnp.float32)
        return [(base * occupied, slope * occupied) for base, slope in absorb]

    row_frac = []
    for t in range(row_tiles):
        frac = jnp.zeros((SUB, LANES), jnp.float32)
        for y in range(SUB):
            frac = jnp.where(sub == y, row_ref[t * SUB + y].astype(jnp.float32), frac)
        row_frac.append(frac / 8.0)

    def row_weights(t):
        if isinstance(t, int):
            frac = row_frac[t]
        else:
            frac = row_frac[-1]
            for i in range(row_tiles - 1):
                frac = jnp.where(t == i, row_frac[i], frac)
        gain = 0.5 * float(levels - 1)
        return gain * (1.0 - frac), gain * frac

    def col_weights(c):
        frac = jnp.broadcast_to(col_ref[c : c + 1, :].astype(jnp.float32) / 8.0, (SUB, LANES))
        keep = 1.0 - frac
        if c == tiles - 1:
            frac = jnp.where(last_lane, 0.0, frac)
        return keep, frac

    def rows_mixed(c, z, at, rw):
        return rw[0] * dens[c, z, pl.ds(at, SUB), :] + rw[1] * dens[c, z, pl.ds(at + 1, SUB), :]

    def cols_mixed(mixed, right_edge, cw):
        turned = pltpu.roll(mixed, LANES - 1, 1)
        return cw[0] * mixed + cw[1] * jnp.where(last_lane, right_edge, turned), turned

    def shade(prev, now, carry, absorb_c):
        through, depth, light = carry
        scaled = prev + now
        knot = lax.round(scaled - 0.5, lax.RoundingMethod.TO_NEAREST_EVEN).astype(jnp.int32)
        low = jnp.bitwise_and(knot, SUB - 1)

        def value(table):
            picked = [(pick(base, low), pick(slope, low)) for base, slope in table]
            base, slope = picked[-1]
            for i in range(len(picked) - 2, -1, -1):
                here = knot < (i + 1) * SUB
                base = jnp.where(here, picked[i][0], base)
                slope = jnp.where(here, picked[i][1], slope)
            return base + slope * scaled

        depth = depth + value(absorb_c)
        after = jnp.exp2(depth)
        light = light + (through - after) * value(emit)
        return after, depth, light

    zero = jnp.zeros((SUB, LANES), jnp.float32)
    one = jnp.ones((SUB, LANES), jnp.float32)

    def march(t):
        at = t * SUB
        if not isinstance(t, int):
            at = pl.multiple_of(at, SUB)
        rw = row_weights(t)
        for z in range(slab):
            edge[z] = zero
        for n, c in enumerate(order):
            if t == row_tiles - 1 and n % group == 0:
                fill_rows(order[n : n + group])
            cw = col_weights(c)
            absorb_c = absorb_of(c)
            carry = (one, zero, zero)
            prev = None
            for z in range(slab):
                now, turned = cols_mixed(rows_mixed(c, z, at, rw), edge[z], cw)
                edge[z] = turned
                if prev is not None:
                    carry = shade(prev, now, carry, absorb_c)
                prev = now
            state[t, c, 0] = prev
            state[t, c, 1] = carry[1]
            state[t, c, 2] = carry[2]

    landed(dens.at[:, pl.ds(1, slab - 1), pl.ds(0, rows), :], load_sem)

    def fill_rows(group_tiles):
        low = group_tiles[-1]

        @pl.when(down_r)
        def _():
            landed(row_halo.at[pl.ds(low, group)], rows_recv_sem.at[low // group])
            for c in group_tiles:
                for z in range(slab):
                    dens[c, z, rows : rows + 1, :] = row_halo[c, z : z + 1, :]

        @pl.when(jnp.logical_not(down_r))
        def _():
            for c in group_tiles:
                for z in range(slab):
                    dens[c, z, rows : rows + 1, :] = jnp.zeros((1, LANES), jnp.float32)

    for t in range(row_tiles):
        march(t)

    @pl.when(both(down_d, down_r))
    def _():
        corner_copy.wait_recv()
        for c in order:
            dens[c, slab, rows : rows + 1, :] = corner[c : c + 1, :]

    @pl.when(both(down_d, jnp.logical_not(down_r)))
    def _():
        for c in order:
            dens[c, slab, rows : rows + 1, :] = jnp.zeros((1, LANES), jnp.float32)

    def owner_of(c):
        return lax.rem(c, owners), c // owners

    def part_copy(c, source, to_slot):
        q, k = owner_of(c)
        return remote(
            parts.at[c],
            gathered.at[to_slot, k, source],
            part_send_sem,
            part_recv_sem.at[to_slot, k],
            (half * members + q, host_row),
        )

    def own_tile(c):
        return both(is_host, m == owner_of(c)[0])

    pl.when(related > earlier)(lambda: pl.semaphore_wait(ready, related - earlier))
    edges = [zero] * row_tiles
    for c in order:
        if (c + 1) % group == 0:

            @pl.when(down_d)
            def _(c=c):
                landed(
                    dens.at[pl.ds(c + 1 - group, group), slab, pl.ds(0, rows), :],
                    depth_recv_sem.at[c // group],
                )

        cw = col_weights(c)
        absorb_c = absorb_of(c)
        for t in range(row_tiles):
            now, edges[t] = cols_mixed(rows_mixed(c, slab, t * SUB, row_weights(t)), edges[t], cw)
            depth = state[t, c, 1]
            carry = (jnp.exp2(depth), depth, state[t, c, 2])
            _, depth, light = shade(state[t, c, 0], now, carry, absorb_c)
            parts[c, 0, t * SUB : (t + 1) * SUB, :] = depth
            parts[c, 1, t * SUB : (t + 1) * SUB, :] = light

        @pl.when(jnp.logical_not(own_tile(c)))
        def _():
            part_copy(c, m, slot).start()

        @pl.when(own_tile(c))
        def _():
            gathered[hosts - 1, c // owners, pl.ds(m, 1)] = parts[pl.ds(c, 1)]

    def pair_copy(s, target, from_half, q, first=0, count=per_owner):
        part = pl.ds(first, count)
        return remote(
            pairs.at[s, part],
            pair_in.at[from_half, q, part],
            pair_send_sem.at[s, target // members],
            pair_recv_sem.at[from_half, q],
            (target, host_row - hosts + 1 + s),
        )

    def factor_copy(s, j, q):
        return remote(
            factors.at[s, j],
            factor_in.at[q],
            factor_send_sem.at[s],
            factor_recv_sem,
            (half * members + j, host_row - hosts + 1 + s),
        )

    def elsewhere(s, j, body):
        if s == hosts - 1:
            pl.when(j != d)(body)
        else:
            body()

    def compose(k, s):
        mine = k * owners + m

        if s == hosts - 1:
            landed(gathered.at[s, k, pl.ds(0, members - 1)], part_recv_sem.at[s, k])
        else:
            landed(gathered.at[s, k], part_recv_sem.at[s, k])

        def add(j, carry):
            total, radiance = carry
            factor = jnp.exp2(total)
            factors[s, j, k] = factor
            return total + gathered[s, k, j, 0], radiance + factor * gathered[s, k, j, 1]

        blank = jnp.zeros((rows, LANES), jnp.float32)
        carry = (blank, blank)
        if members <= 16:
            for j in range(members):
                carry = add(j, carry)
        else:
            carry = lax.fori_loop(0, members, add, carry)
        pairs[s, k, 0] = carry[0]
        pairs[s, k, 1] = carry[1]

        if s == hosts - 1:
            pair_in[half, m, k] = pairs[s, k]
            factor_in[m, k] = factors[s, m, k]

    ahead = 1

    def reply(target):
        j = lax.rem(target, members)
        for s in range(hosts):
            pl.when(half == target // members)(lambda: elsewhere(s, target, factor_copy(s, j, m).start))
            elsewhere(s, target, pair_copy(s, target, half, m).start)

    @pl.when(is_owner)
    def _():
        for k in range(per_owner - 1, -1, -1):
            for s in range(hosts):
                compose(k, s)

            def early(target, k=k):
                for s in range(hosts):
                    elsewhere(s, target, pair_copy(s, target, half, m, k, 1).start)

            repeat(ahead, early)

        def early_factor(target):
            j = lax.rem(target, members)
            for s in range(hosts):
                pl.when(half == target // members)(lambda: elsewhere(s, target, factor_copy(s, j, m).start))

        repeat(ahead, early_factor)
        repeat(n_depth - ahead, lambda i: reply(i + ahead))

    pl.when(is_owner)(lambda: landed(factor_in.at[pl.ds(0, owners - 1)], factor_recv_sem))
    pl.when(jnp.logical_not(is_owner))(lambda: landed(factor_in, factor_recv_sem))
    for q in range(owners - 1, -1, -1):
        for h in range(HALVES):
            itself = both(is_host, d == h * members + q)
            pl.when(jnp.logical_not(itself))(
                functools.partial(landed, pair_in.at[h, q], pair_recv_sem.at[h, q])
            )
        for k in range(per_owner):
            c = k * owners + q
            where = slice(c * LANES, (c + 1) * LANES)
            before = jnp.exp2(pair_in[0, q, k, 0])
            outside = jnp.where(half > 0, before, 1.0)
            front_ref[0, :, where] = outside * factor_in[q, k]
            image_ref[0, :, where] = pair_in[0, q, k, 1] + before * pair_in[1, q, k, 1]
            image_ref[1, :, where] = before * jnp.exp2(pair_in[1, q, k, 0])

    pl.when(up_d)(lambda: landed(dens.at[:, 0, pl.ds(0, rows), :], depth_send_sem))
    pl.when(up_r)(lambda: landed(row_send, rows_send_sem))
    pl.when(both(up_d, up_r))(corner_copy.wait_send)
    pl.when(jnp.logical_not(is_owner))(lambda: landed(parts, part_send_sem))

    @pl.when(is_owner)
    def _():
        landed(parts.at[pl.ds(0, tiles - per_owner)], part_send_sem)
        for s in range(hosts):
            others = members
            if s == hosts - 1:
                others = members - 1
            landed(factors.at[s, pl.ds(0, others)], factor_send_sem.at[s])
            for h in range(HALVES):
                own = both(s == hosts - 1, half == h)
                pl.when(own)(
                    functools.partial(
                        landed, gathered.at[s, :, pl.ds(0, members - 1)], pair_send_sem.at[s, h]
                    )
                )
                pl.when(jnp.logical_not(own))(
                    functools.partial(landed, gathered.at[s], pair_send_sem.at[s, h])
                )


def on_device(n_depth, n_rows, density, bin_of_level, absorb_bins, emit_bins, occupancy, col_offsets, row_offsets):
    slab, rows, cols = density.shape
    tiles = cols // LANES
    row_tiles = rows // SUB
    members = n_depth // HALVES
    hosts = 2 if n_rows % 2 == 0 else 1
    owners = 1
    while owners * 2 <= members and tiles % (owners * 2) == 0:
        owners *= 2
    per_owner = tiles // owners
    groups = tiles // 4 if tiles % 4 == 0 else tiles
    anywhere = pl.BlockSpec(memory_space=pl.ANY)
    vmem = pl.BlockSpec(memory_space=pltpu.VMEM)
    f32, i32 = jnp.float32, jnp.int32
    dma = pltpu.SemaphoreType.DMA
    held = pl.pallas_call(
        functools.partial(kernel, n_depth, n_rows, hosts, owners),
        out_shape=(pltpu.VMEM((1, rows, cols), f32), pltpu.VMEM((2, rows, cols), f32)),
        in_specs=[anywhere] * 7,
        out_specs=(vmem, vmem),
        scratch_shapes=[
            pltpu.VMEM((tiles, slab + 1, rows + SUB, LANES), f32),
            pltpu.SMEM(bin_of_level.shape, i32),
            pltpu.SMEM(absorb_bins.shape, f32),
            pltpu.SMEM(emit_bins.shape, f32),
            pltpu.SMEM(occupancy.shape, i32),
            pltpu.VMEM((tiles, LANES), i32),
            pltpu.SMEM(row_offsets.shape, i32),
            pltpu.VMEM((tiles, slab, LANES), f32),
            pltpu.VMEM((tiles, slab, LANES), f32),
            pltpu.VMEM((tiles, LANES), f32),
            pltpu.VMEM((tiles, LANES), f32),
            pltpu.VMEM((slab, SUB, LANES), f32),
            pltpu.VMEM((row_tiles, tiles, 3, SUB, LANES), f32),
            pltpu.VMEM((tiles, 2, rows, LANES), f32),
            pltpu.VMEM((hosts, per_owner, members, 2, rows, LANES), f32),
            pltpu.VMEM((hosts, members, per_owner, rows, LANES), f32),
            pltpu.VMEM((hosts, per_owner, 2, rows, LANES), f32),
            pltpu.VMEM((owners, per_owner, rows, LANES), f32),
            pltpu.VMEM((HALVES, owners, per_owner, 2, rows, LANES), f32),
            dma,
            dma,
            dma,
            dma((6,)),
            pltpu.SemaphoreType.REGULAR,
            dma,
            dma((groups,)),
            dma,
            dma((groups,)),
            dma((2,)),
            dma,
            dma((hosts, per_owner)),
            dma((hosts,)),
            dma,
            dma((hosts, HALVES)),
            dma((HALVES, owners)),
        ],
        compiler_params=pltpu.CompilerParams(collective_id=0, has_side_effects=True),
    )(
        density,
        bin_of_level,
        absorb_bins,
        emit_bins,
        occupancy,
        col_offsets.reshape(tiles, LANES),
        row_offsets,
    )
    return pl.pallas_call(
        put_out,
        out_shape=(jax.ShapeDtypeStruct((1, rows, cols), f32), jax.ShapeDtypeStruct((2, rows, cols), f32)),
        in_specs=[vmem] * 2,
        out_specs=(anywhere, anywhere),
        scratch_shapes=[dma((2,))],
    )(*(pltpu.with_memory_space_constraint(x, pltpu.VMEM) for x in held))


def put_out(front, image, front_out, image_out, sem):
    copies = [
        pltpu.make_async_copy(front, front_out, sem.at[0]),
        pltpu.make_async_copy(image, image_out, sem.at[1]),
    ]
    for copy in copies:
        copy.start()
    for copy in copies:
        copy.wait()


def solution(mesh):
    placed = (P("depth", "rows", None), P(), P(), P(), P("depth", "rows", None), P(), P("rows"))
    return jax.shard_map(
        functools.partial(on_device, mesh.shape["depth"], mesh.shape["rows"]),
        mesh=mesh,
        in_specs=placed,
        out_specs=(P("depth", "rows", None), P(None, "rows", None)),
        check_vma=False,
    )
```

```python
import functools
import math

import jax
import jax.numpy as jnp
from jax import lax
from jax.experimental import pallas as pl
from jax.experimental.pallas import tpu as pltpu
from jax.sharding import PartitionSpec as P

LANES = 128
SUB = 8
HALVES = 2
MESH = pl.DeviceIdType.MESH


def repeat(count, body):
    if count <= 16:
        for i in range(count):
            body(i)
    else:
        lax.fori_loop(0, count, lambda i, c: (body(i), c)[1], 0)


def pick(table, index):
    dims = lax.GatherDimensionNumbers(
        offset_dims=(),
        collapsed_slice_dims=(0,),
        start_index_map=(0,),
        operand_batching_dims=(1,),
        start_indices_batching_dims=(1,),
    )
    return lax.gather(
        table, index[..., None], dims, slice_sizes=(1, 1), mode=lax.GatherScatterMode.PROMISE_IN_BOUNDS
    )


def both(*conditions):
    return functools.reduce(jnp.logical_and, conditions)


def kernel(
    n_depth,
    n_rows,
    hosts,
    owners,
    dens_hbm,
    bins_hbm,
    absorb_hbm,
    emit_hbm,
    occ_hbm,
    col_hbm,
    row_hbm,
    front_ref,
    image_ref,
    dens,
    bins_ref,
    absorb_ref,
    emit_ref,
    occ_ref,
    col_ref,
    row_ref,
    row_send,
    row_halo,
    corner_send,
    corner,
    edge,
    state,
    parts,
    gathered,
    factors,
    pairs,
    finals,
    crossed,
    factor_in,
    pair_in,
    first_sem,
    rows_sem,
    load_sem,
    small_sem,
    ready,
    depth_send_sem,
    depth_recv_sem,
    rows_send_sem,
    rows_recv_sem,
    corner_sem,
    part_send_sem,
    part_recv_sem,
    factor_send_sem,
    factor_recv_sem,
    pair_send_sem,
    pair_recv_sem,
    cross_sem,
    lead_sem,
):
    slab, rows, cols = dens_hbm.shape
    tiles = cols // LANES
    row_tiles = rows // SUB
    levels = bins_ref.shape[0]
    members = n_depth // HALVES
    per_owner = tiles // owners
    d = lax.axis_index("depth")
    r = lax.axis_index("rows")
    half = d // members
    m = lax.rem(d, members)
    slot = lax.rem(r, hosts)
    host_row = r - slot + hosts - 1
    is_host = slot == hosts - 1
    is_owner = both(is_host, m < owners)

    def first_load(c):
        return pltpu.make_async_copy(
            dens_hbm.at[0, :, pl.ds(c * LANES, LANES)],
            dens.at[c, 0, pl.ds(0, rows), :],
            first_sem,
        )

    def rows_load(c):
        return pltpu.make_async_copy(
            dens_hbm.at[:, 0, pl.ds(c * LANES, LANES)],
            row_send.at[c],
            rows_sem,
        )

    def load(c):
        return pltpu.make_async_copy(
            dens_hbm.at[pl.ds(1, slab - 1), :, pl.ds(c * LANES, LANES)],
            dens.at[c, pl.ds(1, slab - 1), pl.ds(0, rows), :],
            load_sem,
        )

    small = [
        pltpu.make_async_copy(src, dst, small_sem.at[i])
        for i, (src, dst) in enumerate(
            (
                (bins_hbm, bins_ref),
                (absorb_hbm, absorb_ref),
                (emit_hbm, emit_ref),
                (occ_hbm, occ_ref),
                (col_hbm, col_ref),
                (row_hbm, row_ref),
            )
        )
    ]
    def landed(ref, semaphore):
        pltpu.make_async_copy(ref, ref, semaphore).wait()

    barrier = pltpu.get_barrier_semaphore()
    up_d, down_d = d > 0, d < n_depth - 1
    up_r, down_r = r > 0, r < n_rows - 1

    def greet(semaphore, dd, rr):
        pl.semaphore_signal(semaphore, inc=1, device_id=(dd, rr), device_id_type=MESH)

    for there, dd, rr in ((down_d, d + 1, r), (down_r, d, r + 1), (both(down_d, down_r), d + 1, r + 1)):
        pl.when(there)(functools.partial(greet, barrier, dd, rr))

    group = 4 if tiles % 4 == 0 else 1
    order = list(range(tiles - 1, -1, -1))
    for c in order:
        first_load(c).start()
    for c in order:
        rows_load(c).start()
    for c in order:
        load(c).start()
    for copy in small:
        copy.start()

    def greet_block(semaphore, later):
        for s in range(hosts):

            def one(j, s=s):
                wanted = is_owner
                if s == hosts - 1:
                    wanted = jnp.logical_or(wanted, lax.rem(j, members) < owners)
                if later:
                    side = jnp.logical_or(j > d, both(j == d, s > slot))
                else:
                    side = jnp.logical_or(j < d, both(j == d, s < slot))
                pl.when(both(wanted, side))(
                    functools.partial(greet, semaphore, jnp.int32(j), host_row - hosts + 1 + s)
                )

            repeat(n_depth, one)

    greet_block(barrier, True)
    earlier = jnp.where(is_owner, d * hosts + slot, half * owners + jnp.minimum(m, owners))
    related = jnp.where(is_owner, n_depth * hosts - 1, HALVES * owners)
    expected = earlier
    for there in (up_d, up_r, both(up_d, up_r)):
        expected = expected + there.astype(jnp.int32)

    def remote(src, dst, send_sem, recv_sem, device):
        return pltpu.make_async_remote_copy(
            src_ref=src,
            dst_ref=dst,
            send_sem=send_sem,
            recv_sem=recv_sem,
            device_id=device,
            device_id_type=MESH,
        )

    def depth_copy(c):
        return remote(
            dens.at[c, 0, pl.ds(0, rows), :],
            dens.at[c, slab, pl.ds(0, rows), :],
            depth_send_sem,
            depth_recv_sem.at[c // group],
            (d - 1, r),
        )

    def rows_copy(c):
        return remote(row_send.at[c], row_halo.at[c], rows_send_sem, rows_recv_sem.at[c // group], (d, r - 1))

    corner_copy = remote(corner_send, corner, corner_sem.at[0], corner_sem.at[1], (d - 1, r - 1))

    pl.when(expected > 0)(lambda: pl.semaphore_wait(barrier, expected))
    landed(dens.at[:, 0, pl.ds(0, rows), :], first_sem)

    at_once = jnp.logical_or(slot < hosts - 1, hosts == 1)

    def send_depth():
        for c in order:
            depth_copy(c).start()

    pl.when(both(up_d, at_once))(send_depth)

    landed(row_send, rows_sem)
    for c in order:
        corner_send[c : c + 1, :] = row_send[c, 0:1, :]

    @pl.when(up_r)
    def _():
        for c in order:
            rows_copy(c).start()

    greet_block(ready, False)
    pl.when(both(up_d, up_r))(corner_copy.start)

    @pl.when(jnp.logical_not(down_d))
    def _():
        dens[:, slab] = jnp.zeros((tiles,) + dens.shape[2:], jnp.float32)

    lane = lax.broadcasted_iota(jnp.int32, (SUB, LANES), 1)
    sub = lax.broadcasted_iota(jnp.int32, (SUB, LANES), 0)
    last_lane = lane == LANES - 1

    for copy in small:
        copy.wait()

    def tables(values):
        values = values + values[-1:]
        out = []
        for first in range(0, levels, SUB):
            base = jnp.zeros((SUB, LANES), jnp.float32)
            slope = jnp.zeros((SUB, LANES), jnp.float32)
            for k in range(first, min(first + SUB, levels)):
                step = values[k + 1] - values[k]
                base = jnp.where(sub == k - first, values[k] - step * float(k), base)
                slope = jnp.where(sub == k - first, step, slope)
            out.append((base, slope))
        return out

    to_log2 = -math.log2(math.e)
    absorb = tables([absorb_ref[bins_ref[k]] * to_log2 for k in range(levels)])
    emit = tables([emit_ref[bins_ref[k]] for k in range(levels)])

    def absorb_of(c):
        occupied = occ_ref[0, 0, (c * LANES) // (cols // occ_ref.shape[2])].astype(jnp.float32)
        return [(base * occupied, slope * occupied) for base, slope in absorb]

    row_frac = []
    for t in range(row_tiles):
        frac = jnp.zeros((SUB, LANES), jnp.float32)
        for y in range(SUB):
            frac = jnp.where(sub == y, row_ref[t * SUB + y].astype(jnp.float32), frac)
        row_frac.append(frac / 8.0)

    def row_weights(t):
        if isinstance(t, int):
            frac = row_frac[t]
        else:
            frac = row_frac[-1]
            for i in range(row_tiles - 1):
                frac = jnp.where(t == i, row_frac[i], frac)
        gain = 0.5 * float(levels - 1)
        return gain * (1.0 - frac), gain * frac

    def col_weights(c):
        frac = jnp.broadcast_to(col_ref[c : c + 1, :].astype(jnp.float32) / 8.0, (SUB, LANES))
        keep = 1.0 - frac
        if c == tiles - 1:
            frac = jnp.where(last_lane, 0.0, frac)
        return keep, frac

    def rows_mixed(c, z, at, rw):
        return rw[0] * dens[c, z, pl.ds(at, SUB), :] + rw[1] * dens[c, z, pl.ds(at + 1, SUB), :]

    def cols_mixed(mixed, right_edge, cw):
        turned = pltpu.roll(mixed, LANES - 1, 1)
        return cw[0] * mixed + cw[1] * jnp.where(last_lane, right_edge, turned), turned

    def shade(prev, now, carry, absorb_c):
        through, depth, light = carry
        scaled = prev + now
        knot = lax.round(scaled - 0.5, lax.RoundingMethod.TO_NEAREST_EVEN).astype(jnp.int32)
        low = jnp.bitwise_and(knot, SUB - 1)

        def value(table):
            picked = [(pick(base, low), pick(slope, low)) for base, slope in table]
            base, slope = picked[-1]
            for i in range(len(picked) - 2, -1, -1):
                here = knot < (i + 1) * SUB
                base = jnp.where(here, picked[i][0], base)
                slope = jnp.where(here, picked[i][1], slope)
            return base + slope * scaled

        depth = depth + value(absorb_c)
        after = jnp.exp2(depth)
        light = light + (through - after) * value(emit)
        return after, depth, light

    zero = jnp.zeros((SUB, LANES), jnp.float32)
    one = jnp.ones((SUB, LANES), jnp.float32)

    def march(t):
        at = t * SUB
        if not isinstance(t, int):
            at = pl.multiple_of(at, SUB)
        rw = row_weights(t)
        for z in range(slab):
            edge[z] = zero
        for n, c in enumerate(order):
            if t == row_tiles - 1 and n % group == 0:
                fill_rows(order[n : n + group])
            cw = col_weights(c)
            absorb_c = absorb_of(c)
            carry = (one, zero, zero)
            prev = None
            for z in range(slab):
                now, turned = cols_mixed(rows_mixed(c, z, at, rw), edge[z], cw)
                edge[z] = turned
                if prev is not None:
                    carry = shade(prev, now, carry, absorb_c)
                prev = now
            state[t, c, 0] = prev
            state[t, c, 1] = carry[1]
            state[t, c, 2] = carry[2]

    landed(dens.at[:, pl.ds(1, slab - 1), pl.ds(0, rows), :], load_sem)

    def fill_rows(group_tiles):
        low = group_tiles[-1]

        @pl.when(down_r)
        def _():
            landed(row_halo.at[pl.ds(low, group)], rows_recv_sem.at[low // group])
            for c in group_tiles:
                for z in range(slab):
                    dens[c, z, rows : rows + 1, :] = row_halo[c, z : z + 1, :]

        @pl.when(jnp.logical_not(down_r))
        def _():
            for c in group_tiles:
                for z in range(slab):
                    dens[c, z, rows : rows + 1, :] = jnp.zeros((1, LANES), jnp.float32)

    for t in range(row_tiles):
        march(t)
        if t == 0:
            pl.when(both(up_d, jnp.logical_not(at_once)))(send_depth)

    @pl.when(both(down_d, down_r))
    def _():
        corner_copy.wait_recv()
        for c in order:
            dens[c, slab, rows : rows + 1, :] = corner[c : c + 1, :]

    @pl.when(both(down_d, jnp.logical_not(down_r)))
    def _():
        for c in order:
            dens[c, slab, rows : rows + 1, :] = jnp.zeros((1, LANES), jnp.float32)

    def owner_of(c):
        return lax.rem(c, owners), c // owners

    def part_copy(c, source, to_slot):
        q, k = owner_of(c)
        return remote(
            parts.at[c],
            gathered.at[to_slot, k, source],
            part_send_sem,
            part_recv_sem.at[to_slot, k],
            (half * members + q, host_row),
        )

    def own_tile(c):
        return both(is_host, m == owner_of(c)[0])

    pl.when(related > earlier)(lambda: pl.semaphore_wait(ready, related - earlier))
    edges = [zero] * row_tiles
    for c in order:
        if (c + 1) % group == 0:

            @pl.when(down_d)
            def _(c=c):
                landed(
                    dens.at[pl.ds(c + 1 - group, group), slab, pl.ds(0, rows), :],
                    depth_recv_sem.at[c // group],
                )

        cw = col_weights(c)
        absorb_c = absorb_of(c)
        for t in range(row_tiles):
            now, edges[t] = cols_mixed(rows_mixed(c, slab, t * SUB, row_weights(t)), edges[t], cw)
            depth = state[t, c, 1]
            carry = (jnp.exp2(depth), depth, state[t, c, 2])
            _, depth, light = shade(state[t, c, 0], now, carry, absorb_c)
            parts[c, 0, t * SUB : (t + 1) * SUB, :] = depth
            parts[c, 1, t * SUB : (t + 1) * SUB, :] = light

        @pl.when(jnp.logical_not(own_tile(c)))
        def _():
            part_copy(c, m, slot).start()

        @pl.when(own_tile(c))
        def _():
            gathered[hosts - 1, c // owners, pl.ds(m, 1)] = parts[pl.ds(c, 1)]

    def pair_copy(s, target, from_half, q, first=0, count=per_owner, send_sem=None):
        part = pl.ds(first, count)
        return remote(
            pairs.at[s, part],
            pair_in.at[from_half, q, part],
            pair_send_sem.at[s, 0] if send_sem is None else send_sem,
            pair_recv_sem.at[from_half, q],
            (target, host_row - hosts + 1 + s),
        )

    def factor_copy(s, j, q):
        return remote(
            factors.at[s, j],
            factor_in.at[q],
            factor_send_sem.at[s],
            factor_recv_sem,
            (half * members + j, host_row - hosts + 1 + s),
        )

    def elsewhere(s, j, body):
        if s == hosts - 1:
            pl.when(j != d)(body)
        else:
            body()

    def compose(k, s):
        mine = k * owners + m

        if s == hosts - 1:
            landed(gathered.at[s, k, pl.ds(0, members - 1)], part_recv_sem.at[s, k])
        else:
            landed(gathered.at[s, k], part_recv_sem.at[s, k])

        def add(j, carry):
            total, radiance = carry
            factor = jnp.exp2(total)
            factors[s, j, k] = factor
            return total + gathered[s, k, j, 0], radiance + factor * gathered[s, k, j, 1]

        blank = jnp.zeros((rows, LANES), jnp.float32)
        carry = (blank, blank)
        if members <= 16:
            for j in range(members):
                carry = add(j, carry)
        else:
            carry = lax.fori_loop(0, members, add, carry)
        pairs[s, k, 0] = carry[0]
        pairs[s, k, 1] = carry[1]

        if s == hosts - 1:

            @pl.when(half == 0)
            def _():
                pair_in[0, m, k] = pairs[s, k]
                factor_in[m, k] = factors[s, m, k]

    def reply_factor(target):
        j = lax.rem(target, members)
        for s in range(hosts):
            elsewhere(s, half * members + j, factor_copy(s, j, m).start)

    def reply(target, first=0, count=per_owner):
        for s in range(hosts):
            elsewhere(s, target, pair_copy(s, target, half, m, first, count).start)

    def lead(k):
        for s in range(hosts):
            elsewhere(s, 0, pair_copy(s, 0, half, m, k, 1, lead_sem.at[s]).start)

    def led():
        for s in range(hosts):
            elsewhere(s, 0, functools.partial(landed, pairs.at[s], lead_sem.at[s]))

    def cross_copy(s):
        return remote(
            pairs.at[s],
            crossed.at[s],
            pair_send_sem.at[s, 1],
            cross_sem.at[s],
            (members + m, host_row),
        )

    def final_copy(s, j):
        return remote(
            finals.at[s],
            pair_in.at[1, m],
            pair_send_sem.at[s, 1],
            pair_recv_sem.at[1, m],
            (members + j, host_row - hosts + 1 + s),
        )

    def front_half():
        reply_factor(0)
        for s in range(hosts):
            cross_copy(s).start()

        def one(i):
            reply_factor(i + 1)
            reply(i + 1)

        repeat(members - 1, one)

    def back_half():
        led()
        split = (members - 1, members - 2) if members > 2 and False else ()
        repeat(members - len(split) - 1, lambda i: reply(i + 1))
        for k in range(per_owner - 1, -1, -1):
            for target in split:
                reply(target, k, 1)
        for s in range(hosts):
            landed(crossed.at[s], cross_sem.at[s])
            for k in range(per_owner):
                before = jnp.exp2(crossed[s, k, 0])
                finals[s, k, 0] = crossed[s, k, 1] + before * pairs[s, k, 1]
                finals[s, k, 1] = before * jnp.exp2(pairs[s, k, 0])

                def scale(j, s=s, k=k, before=before):
                    factors[s, j, k] = before * factors[s, j, k]

                repeat(members, scale)

            if s == hosts - 1:
                pair_in[1, m] = finals[s]
                factor_in[m] = factors[s, m]

            def give(j, s=s):
                elsewhere(s, members + j, final_copy(s, j).start)
                elsewhere(s, members + j, factor_copy(s, j, m).start)

            repeat(members, give)

    @pl.when(is_owner)
    def _():
        for k in range(per_owner - 1, -1, -1):
            for s in range(hosts):
                compose(k, s)
            lead(k)
        pl.when(half == 0)(front_half)
        pl.when(half == 1)(back_half)

    pl.when(is_owner)(lambda: landed(factor_in.at[pl.ds(0, owners - 1)], factor_recv_sem))
    pl.when(jnp.logical_not(is_owner))(lambda: landed(factor_in, factor_recv_sem))
    for q in range(owners):
        for h in range(HALVES):
            needed = jnp.logical_not(both(is_host, d == h * members + q))
            if h == 0:
                needed = both(needed, half == 0)
            pl.when(needed)(functools.partial(landed, pair_in.at[h, q], pair_recv_sem.at[h, q]))

        @pl.when(half == 0)
        def _(q=q):
            for k in range(per_owner):
                c = k * owners + q
                where = slice(c * LANES, (c + 1) * LANES)
                before = jnp.exp2(pair_in[0, q, k, 0])
                front_ref[0, :, where] = factor_in[q, k]
                image_ref[0, :, where] = pair_in[0, q, k, 1] + before * pair_in[1, q, k, 1]
                image_ref[1, :, where] = before * jnp.exp2(pair_in[1, q, k, 0])

        @pl.when(half == 1)
        def _(q=q):
            for k in range(per_owner):
                c = k * owners + q
                where = slice(c * LANES, (c + 1) * LANES)
                front_ref[0, :, where] = factor_in[q, k]
                image_ref[0, :, where] = pair_in[1, q, k, 0]
                image_ref[1, :, where] = pair_in[1, q, k, 1]

    pl.when(up_d)(lambda: landed(dens.at[:, 0, pl.ds(0, rows), :], depth_send_sem))
    pl.when(up_r)(lambda: landed(row_send, rows_send_sem))
    pl.when(both(up_d, up_r))(corner_copy.wait_send)
    pl.when(jnp.logical_not(is_owner))(lambda: landed(parts, part_send_sem))

    @pl.when(is_owner)
    def _():
        landed(parts.at[pl.ds(0, tiles - per_owner)], part_send_sem)
        for s in range(hosts):
            others = members
            if s == hosts - 1:
                others = members - 1
            landed(factors.at[s, pl.ds(0, others)], factor_send_sem.at[s])

            @pl.when(half == 0)
            def _(s=s):
                if s < hosts - 1:
                    landed(gathered.at[s, :, pl.ds(0, members - 1)], pair_send_sem.at[s, 0])
                else:
                    pl.when(d == 0)(
                        lambda: landed(gathered.at[s, :, pl.ds(0, members - 1)], pair_send_sem.at[s, 0])
                    )
                    pl.when(d > 0)(
                        lambda: landed(gathered.at[s, :, pl.ds(0, members - 2)], pair_send_sem.at[s, 0])
                    )
                landed(pairs.at[s], pair_send_sem.at[s, 1])

            @pl.when(half == 1)
            def _(s=s, others=others):
                landed(gathered.at[s, :, pl.ds(0, members - 1)], pair_send_sem.at[s, 0])
                landed(gathered.at[s, :, pl.ds(0, others)], pair_send_sem.at[s, 1])

        pl.when(half == 0)(led)


def on_device(n_depth, n_rows, density, bin_of_level, absorb_bins, emit_bins, occupancy, col_offsets, row_offsets):
    slab, rows, cols = density.shape
    tiles = cols // LANES
    row_tiles = rows // SUB
    members = n_depth // HALVES
    hosts = 2 if n_rows % 2 == 0 else 1
    owners = 1
    while owners * 2 <= members and tiles % (owners * 2) == 0:
        owners *= 2
    per_owner = tiles // owners
    groups = tiles // 4 if tiles % 4 == 0 else tiles
    anywhere = pl.BlockSpec(memory_space=pl.ANY)
    vmem = pl.BlockSpec(memory_space=pltpu.VMEM)
    f32, i32 = jnp.float32, jnp.int32
    dma = pltpu.SemaphoreType.DMA
    held = pl.pallas_call(
        functools.partial(kernel, n_depth, n_rows, hosts, owners),
        out_shape=(pltpu.VMEM((1, rows, cols), f32), pltpu.VMEM((2, rows, cols), f32)),
        in_specs=[anywhere] * 7,
        out_specs=(vmem, vmem),
        scratch_shapes=[
            pltpu.VMEM((tiles, slab + 1, rows + SUB, LANES), f32),
            pltpu.SMEM(bin_of_level.shape, i32),
            pltpu.SMEM(absorb_bins.shape, f32),
            pltpu.SMEM(emit_bins.shape, f32),
            pltpu.SMEM(occupancy.shape, i32),
            pltpu.VMEM((tiles, LANES), i32),
            pltpu.SMEM(row_offsets.shape, i32),
            pltpu.VMEM((tiles, slab, LANES), f32),
            pltpu.VMEM((tiles, slab, LANES), f32),
            pltpu.VMEM((tiles, LANES), f32),
            pltpu.VMEM((tiles, LANES), f32),
            pltpu.VMEM((slab, SUB, LANES), f32),
            pltpu.VMEM((row_tiles, tiles, 3, SUB, LANES), f32),
            pltpu.VMEM((tiles, 2, rows, LANES), f32),
            pltpu.VMEM((hosts, per_owner, members, 2, rows, LANES), f32),
            pltpu.VMEM((hosts, members, per_owner, rows, LANES), f32),
            pltpu.VMEM((hosts, per_owner, 2, rows, LANES), f32),
            pltpu.VMEM((hosts, per_owner, 2, rows, LANES), f32),
            pltpu.VMEM((hosts, per_owner, 2, rows, LANES), f32),
            pltpu.VMEM((owners, per_owner, rows, LANES), f32),
            pltpu.VMEM((HALVES, owners, per_owner, 2, rows, LANES), f32),
            dma,
            dma,
            dma,
            dma((6,)),
            pltpu.SemaphoreType.REGULAR,
            dma,
            dma((groups,)),
            dma,
            dma((groups,)),
            dma((2,)),
            dma,
            dma((hosts, per_owner)),
            dma((hosts,)),
            dma,
            dma((hosts, HALVES)),
            dma((HALVES, owners)),
            dma((hosts,)),
            dma((hosts,)),
        ],
        compiler_params=pltpu.CompilerParams(collective_id=0, has_side_effects=True),
    )(
        density,
        bin_of_level,
        absorb_bins,
        emit_bins,
        occupancy,
        col_offsets.reshape(tiles, LANES),
        row_offsets,
    )
    return pl.pallas_call(
        put_out,
        out_shape=(jax.ShapeDtypeStruct((1, rows, cols), f32), jax.ShapeDtypeStruct((2, rows, cols), f32)),
        in_specs=[vmem] * 2,
        out_specs=(anywhere, anywhere),
        scratch_shapes=[dma((2,))],
    )(*(pltpu.with_memory_space_constraint(x, pltpu.VMEM) for x in held))


def put_out(front, image, front_out, image_out, sem):
    copies = [
        pltpu.make_async_copy(front, front_out, sem.at[0]),
        pltpu.make_async_copy(image, image_out, sem.at[1]),
    ]
    for copy in copies:
        copy.start()
    for copy in copies:
        copy.wait()


def solution(mesh):
    placed = (P("depth", "rows", None), P(), P(), P(), P("depth", "rows", None), P(), P("rows"))
    return jax.shard_map(
        functools.partial(on_device, mesh.shape["depth"], mesh.shape["rows"]),
        mesh=mesh,
        in_specs=placed,
        out_specs=(P("depth", "rows", None), P(None, "rows", None)),
        check_vma=False,
    )
```

```python
import functools
import math

import jax
import jax.numpy as jnp
from jax import lax
from jax.experimental import pallas as pl
from jax.experimental.pallas import tpu as pltpu
from jax.sharding import PartitionSpec as P

LANES = 128
SUB = 8
HALVES = 2
MESH = pl.DeviceIdType.MESH


def repeat(count, body):
    if count <= 16:
        for i in range(count):
            body(i)
    else:
        lax.fori_loop(0, count, lambda i, c: (body(i), c)[1], 0)


def pick(table, index):
    dims = lax.GatherDimensionNumbers(
        offset_dims=(),
        collapsed_slice_dims=(0,),
        start_index_map=(0,),
        operand_batching_dims=(1,),
        start_indices_batching_dims=(1,),
    )
    return lax.gather(
        table, index[..., None], dims, slice_sizes=(1, 1), mode=lax.GatherScatterMode.PROMISE_IN_BOUNDS
    )


def both(*conditions):
    return functools.reduce(jnp.logical_and, conditions)


def kernel(
    n_depth,
    n_rows,
    hosts,
    owners,
    dens_hbm,
    bins_hbm,
    absorb_hbm,
    emit_hbm,
    occ_hbm,
    col_hbm,
    row_hbm,
    front_ref,
    image_ref,
    dens,
    bins_ref,
    absorb_ref,
    emit_ref,
    occ_ref,
    col_ref,
    row_ref,
    row_send,
    row_halo,
    corner_send,
    corner,
    edge,
    state,
    parts,
    gathered,
    factors,
    pairs,
    finals,
    crossed,
    factor_in,
    pair_in,
    first_sem,
    rows_sem,
    load_sem,
    small_sem,
    ready,
    depth_send_sem,
    depth_recv_sem,
    rows_send_sem,
    rows_recv_sem,
    corner_sem,
    part_send_sem,
    part_recv_sem,
    factor_send_sem,
    factor_recv_sem,
    pair_send_sem,
    pair_recv_sem,
    cross_sem,
    lead_sem,
):
    slab, rows, cols = dens_hbm.shape
    tiles = cols // LANES
    row_tiles = rows // SUB
    levels = bins_ref.shape[0]
    members = n_depth // HALVES
    per_owner = tiles // owners
    d = lax.axis_index("depth")
    r = lax.axis_index("rows")
    half = d // members
    m = lax.rem(d, members)
    slot = lax.rem(r, hosts)
    host_row = r - slot + hosts - 1
    is_host = slot == hosts - 1
    is_owner = both(is_host, m < owners)

    def first_load(c):
        return pltpu.make_async_copy(
            dens_hbm.at[0, :, pl.ds(c * LANES, LANES)],
            dens.at[c, 0, pl.ds(0, rows), :],
            first_sem,
        )

    def rows_load(c):
        return pltpu.make_async_copy(
            dens_hbm.at[:, 0, pl.ds(c * LANES, LANES)],
            row_send.at[c],
            rows_sem,
        )

    def load(c):
        return pltpu.make_async_copy(
            dens_hbm.at[pl.ds(1, slab - 1), :, pl.ds(c * LANES, LANES)],
            dens.at[c, pl.ds(1, slab - 1), pl.ds(0, rows), :],
            load_sem,
        )

    small = [
        pltpu.make_async_copy(src, dst, small_sem.at[i])
        for i, (src, dst) in enumerate(
            (
                (bins_hbm, bins_ref),
                (absorb_hbm, absorb_ref),
                (emit_hbm, emit_ref),
                (occ_hbm, occ_ref),
                (col_hbm, col_ref),
                (row_hbm, row_ref),
            )
        )
    ]
    def landed(ref, semaphore):
        pltpu.make_async_copy(ref, ref, semaphore).wait()

    barrier = pltpu.get_barrier_semaphore()
    up_d, down_d = d > 0, d < n_depth - 1
    up_r, down_r = r > 0, r < n_rows - 1

    def greet(semaphore, dd, rr):
        pl.semaphore_signal(semaphore, inc=1, device_id=(dd, rr), device_id_type=MESH)

    for there, dd, rr in ((down_d, d + 1, r), (down_r, d, r + 1), (both(down_d, down_r), d + 1, r + 1)):
        pl.when(there)(functools.partial(greet, barrier, dd, rr))

    group = 2 if tiles % 2 == 0 else 1
    order = list(range(tiles - 1, -1, -1))
    for c in order:
        first_load(c).start()
    for c in order:
        rows_load(c).start()
    for c in order:
        load(c).start()
    for copy in small:
        copy.start()

    def greet_block(semaphore, later):
        for s in range(hosts):

            def one(j, s=s):
                wanted = is_owner
                if s == hosts - 1:
                    wanted = jnp.logical_or(wanted, lax.rem(j, members) < owners)
                if later:
                    side = jnp.logical_or(j > d, both(j == d, s > slot))
                else:
                    side = jnp.logical_or(j < d, both(j == d, s < slot))
                pl.when(both(wanted, side))(
                    functools.partial(greet, semaphore, jnp.int32(j), host_row - hosts + 1 + s)
                )

            repeat(n_depth, one)

    greet_block(barrier, True)
    earlier = jnp.where(is_owner, d * hosts + slot, half * owners + jnp.minimum(m, owners))
    related = jnp.where(is_owner, n_depth * hosts - 1, HALVES * owners)
    expected = earlier
    for there in (up_d, up_r, both(up_d, up_r)):
        expected = expected + there.astype(jnp.int32)

    def remote(src, dst, send_sem, recv_sem, device):
        return pltpu.make_async_remote_copy(
            src_ref=src,
            dst_ref=dst,
            send_sem=send_sem,
            recv_sem=recv_sem,
            device_id=device,
            device_id_type=MESH,
        )

    def depth_copy(c):
        return remote(
            dens.at[c, 0, pl.ds(0, rows), :],
            dens.at[c, slab, pl.ds(0, rows), :],
            depth_send_sem,
            depth_recv_sem.at[c // group],
            (d - 1, r),
        )

    def rows_copy(c):
        return remote(row_send.at[c], row_halo.at[c], rows_send_sem, rows_recv_sem.at[c // group], (d, r - 1))

    corner_copy = remote(corner_send, corner, corner_sem.at[0], corner_sem.at[1], (d - 1, r - 1))

    pl.when(expected > 0)(lambda: pl.semaphore_wait(barrier, expected))
    landed(dens.at[:, 0, pl.ds(0, rows), :], first_sem)

    at_once = jnp.logical_or(slot < hosts - 1, hosts == 1)

    def send_depth():
        for c in order:
            depth_copy(c).start()

    pl.when(both(up_d, at_once))(send_depth)

    landed(row_send, rows_sem)
    for c in order:
        corner_send[c : c + 1, :] = row_send[c, 0:1, :]

    @pl.when(up_r)
    def _():
        for c in order:
            rows_copy(c).start()

    greet_block(ready, False)
    pl.when(both(up_d, up_r))(corner_copy.start)

    @pl.when(jnp.logical_not(down_d))
    def _():
        dens[:, slab] = jnp.zeros((tiles,) + dens.shape[2:], jnp.float32)

    lane = lax.broadcasted_iota(jnp.int32, (SUB, LANES), 1)
    sub = lax.broadcasted_iota(jnp.int32, (SUB, LANES), 0)
    last_lane = lane == LANES - 1

    for copy in small:
        copy.wait()

    def tables(values):
        values = values + values[-1:]
        out = []
        for first in range(0, levels, SUB):
            base = jnp.zeros((SUB, LANES), jnp.float32)
            slope = jnp.zeros((SUB, LANES), jnp.float32)
            for k in range(first, min(first + SUB, levels)):
                step = values[k + 1] - values[k]
                base = jnp.where(sub == k - first, values[k] - step * float(k), base)
                slope = jnp.where(sub == k - first, step, slope)
            out.append((base, slope))
        return out

    to_log2 = -math.log2(math.e)
    absorb = tables([absorb_ref[bins_ref[k]] * to_log2 for k in range(levels)])
    emit = tables([emit_ref[bins_ref[k]] for k in range(levels)])

    def absorb_of(c):
        occupied = occ_ref[0, 0, (c * LANES) // (cols // occ_ref.shape[2])].astype(jnp.float32)
        return [(base * occupied, slope * occupied) for base, slope in absorb]

    row_frac = []
    for t in range(row_tiles):
        frac = jnp.zeros((SUB, LANES), jnp.float32)
        for y in range(SUB):
            frac = jnp.where(sub == y, row_ref[t * SUB + y].astype(jnp.float32), frac)
        row_frac.append(frac / 8.0)

    def row_weights(t):
        if isinstance(t, int):
            frac = row_frac[t]
        else:
            frac = row_frac[-1]
            for i in range(row_tiles - 1):
                frac = jnp.where(t == i, row_frac[i], frac)
        gain = 0.5 * float(levels - 1)
        return gain * (1.0 - frac), gain * frac

    def col_weights(c):
        frac = jnp.broadcast_to(col_ref[c : c + 1, :].astype(jnp.float32) / 8.0, (SUB, LANES))
        keep = 1.0 - frac
        if c == tiles - 1:
            frac = jnp.where(last_lane, 0.0, frac)
        return keep, frac

    def rows_mixed(c, z, at, rw):
        return rw[0] * dens[c, z, pl.ds(at, SUB), :] + rw[1] * dens[c, z, pl.ds(at + 1, SUB), :]

    def cols_mixed(mixed, right_edge, cw):
        turned = pltpu.roll(mixed, LANES - 1, 1)
        return cw[0] * mixed + cw[1] * jnp.where(last_lane, right_edge, turned), turned

    def shade(prev, now, carry, absorb_c):
        through, depth, light = carry
        scaled = prev + now
        knot = lax.round(scaled - 0.5, lax.RoundingMethod.TO_NEAREST_EVEN).astype(jnp.int32)
        low = jnp.bitwise_and(knot, SUB - 1)

        def value(table):
            picked = [(pick(base, low), pick(slope, low)) for base, slope in table]
            base, slope = picked[-1]
            for i in range(len(picked) - 2, -1, -1):
                here = knot < (i + 1) * SUB
                base = jnp.where(here, picked[i][0], base)
                slope = jnp.where(here, picked[i][1], slope)
            return base + slope * scaled

        depth = depth + value(absorb_c)
        after = jnp.exp2(depth)
        light = light + (through - after) * value(emit)
        return after, depth, light

    zero = jnp.zeros((SUB, LANES), jnp.float32)
    one = jnp.ones((SUB, LANES), jnp.float32)

    def march(t):
        at = t * SUB
        if not isinstance(t, int):
            at = pl.multiple_of(at, SUB)
        rw = row_weights(t)
        for z in range(slab):
            edge[z] = zero
        for n, c in enumerate(order):
            if t == row_tiles - 1 and n % group == 0:
                fill_rows(order[n : n + group])
            cw = col_weights(c)
            absorb_c = absorb_of(c)
            carry = (one, zero, zero)
            prev = None
            for z in range(slab):
                now, turned = cols_mixed(rows_mixed(c, z, at, rw), edge[z], cw)
                edge[z] = turned
                if prev is not None:
                    carry = shade(prev, now, carry, absorb_c)
                prev = now
            state[t, c, 0] = prev
            state[t, c, 1] = carry[1]
            state[t, c, 2] = carry[2]

    landed(dens.at[:, pl.ds(1, slab - 1), pl.ds(0, rows), :], load_sem)

    def fill_rows(group_tiles):
        low = group_tiles[-1]

        @pl.when(down_r)
        def _():
            landed(row_halo.at[pl.ds(low, group)], rows_recv_sem.at[low // group])
            for c in group_tiles:
                for z in range(slab):
                    dens[c, z, rows : rows + 1, :] = row_halo[c, z : z + 1, :]

        @pl.when(jnp.logical_not(down_r))
        def _():
            for c in group_tiles:
                for z in range(slab):
                    dens[c, z, rows : rows + 1, :] = jnp.zeros((1, LANES), jnp.float32)

    for t in range(row_tiles):
        march(t)
        if t == 0:
            pl.when(both(up_d, jnp.logical_not(at_once)))(send_depth)

    @pl.when(both(down_d, down_r))
    def _():
        corner_copy.wait_recv()
        for c in order:
            dens[c, slab, rows : rows + 1, :] = corner[c : c + 1, :]

    @pl.when(both(down_d, jnp.logical_not(down_r)))
    def _():
        for c in order:
            dens[c, slab, rows : rows + 1, :] = jnp.zeros((1, LANES), jnp.float32)

    def owner_of(c):
        return lax.rem(c, owners), c // owners

    def part_copy(c, source, to_slot):
        q, k = owner_of(c)
        return remote(
            parts.at[c],
            gathered.at[to_slot, k, source],
            part_send_sem,
            part_recv_sem.at[to_slot, k],
            (half * members + q, host_row),
        )

    def own_tile(c):
        return both(is_host, m == owner_of(c)[0])

    pl.when(related > earlier)(lambda: pl.semaphore_wait(ready, related - earlier))
    edges = [zero] * row_tiles
    for c in order:
        if (c + 1) % group == 0:

            @pl.when(down_d)
            def _(c=c):
                landed(
                    dens.at[pl.ds(c + 1 - group, group), slab, pl.ds(0, rows), :],
                    depth_recv_sem.at[c // group],
                )

        cw = col_weights(c)
        absorb_c = absorb_of(c)
        for t in range(row_tiles):
            now, edges[t] = cols_mixed(rows_mixed(c, slab, t * SUB, row_weights(t)), edges[t], cw)
            depth = state[t, c, 1]
            carry = (jnp.exp2(depth), depth, state[t, c, 2])
            _, depth, light = shade(state[t, c, 0], now, carry, absorb_c)
            parts[c, 0, t * SUB : (t + 1) * SUB, :] = depth
            parts[c, 1, t * SUB : (t + 1) * SUB, :] = light

        @pl.when(jnp.logical_not(own_tile(c)))
        def _():
            part_copy(c, m, slot).start()

        @pl.when(own_tile(c))
        def _():
            gathered[hosts - 1, c // owners, pl.ds(m, 1)] = parts[pl.ds(c, 1)]

    def pair_copy(s, target, from_half, q, first=0, count=per_owner, send_sem=None):
        part = pl.ds(first, count)
        return remote(
            pairs.at[s, part],
            pair_in.at[from_half, q, part],
            pair_send_sem.at[s, 0] if send_sem is None else send_sem,
            pair_recv_sem.at[from_half, q],
            (target, host_row - hosts + 1 + s),
        )

    def factor_copy(s, j, q):
        return remote(
            factors.at[s, j],
            factor_in.at[q],
            factor_send_sem.at[s],
            factor_recv_sem,
            (half * members + j, host_row - hosts + 1 + s),
        )

    def elsewhere(s, j, body):
        if s == hosts - 1:
            pl.when(j != d)(body)
        else:
            body()

    def compose(k, s):
        mine = k * owners + m

        if s == hosts - 1:
            landed(gathered.at[s, k, pl.ds(0, members - 1)], part_recv_sem.at[s, k])
        else:
            landed(gathered.at[s, k], part_recv_sem.at[s, k])

        def add(j, carry):
            total, radiance = carry
            factor = jnp.exp2(total)
            factors[s, j, k] = factor
            return total + gathered[s, k, j, 0], radiance + factor * gathered[s, k, j, 1]

        blank = jnp.zeros((rows, LANES), jnp.float32)
        carry = (blank, blank)
        if members <= 16:
            for j in range(members):
                carry = add(j, carry)
        else:
            carry = lax.fori_loop(0, members, add, carry)
        pairs[s, k, 0] = carry[0]
        pairs[s, k, 1] = carry[1]

        if s == hosts - 1:

            @pl.when(half == 0)
            def _():
                pair_in[0, m, k] = pairs[s, k]
                factor_in[m, k] = factors[s, m, k]

    def reply_factor(target):
        j = lax.rem(target, members)
        for s in range(hosts):
            elsewhere(s, half * members + j, factor_copy(s, j, m).start)

    def reply(target, first=0, count=per_owner):
        for s in range(hosts):
            elsewhere(s, target, pair_copy(s, target, half, m, first, count).start)

    def lead(k):
        for s in range(hosts):
            elsewhere(s, 0, pair_copy(s, 0, half, m, k, 1, lead_sem.at[s]).start)

    def led():
        for s in range(hosts):
            elsewhere(s, 0, functools.partial(landed, pairs.at[s], lead_sem.at[s]))

    def cross_copy(s):
        return remote(
            pairs.at[s],
            crossed.at[s],
            pair_send_sem.at[s, 1],
            cross_sem.at[s],
            (members + m, host_row),
        )

    def final_copy(s, j):
        return remote(
            finals.at[s],
            pair_in.at[1, m],
            pair_send_sem.at[s, 1],
            pair_recv_sem.at[1, m],
            (members + j, host_row - hosts + 1 + s),
        )

    def front_half():
        reply_factor(0)
        for s in range(hosts):
            cross_copy(s).start()

        def one(i):
            reply_factor(i + 1)
            reply(i + 1)

        repeat(members - 1, one)

    def back_half():
        led()
        split = (members - 1, members - 2) if members > 2 and False else ()
        repeat(members - len(split) - 1, lambda i: reply(i + 1))
        for k in range(per_owner - 1, -1, -1):
            for target in split:
                reply(target, k, 1)
        for s in range(hosts):
            landed(crossed.at[s], cross_sem.at[s])
            for k in range(per_owner):
                before = jnp.exp2(crossed[s, k, 0])
                finals[s, k, 0] = crossed[s, k, 1] + before * pairs[s, k, 1]
                finals[s, k, 1] = before * jnp.exp2(pairs[s, k, 0])

                def scale(j, s=s, k=k, before=before):
                    factors[s, j, k] = before * factors[s, j, k]

                repeat(members, scale)

            if s == hosts - 1:
                pair_in[1, m] = finals[s]
                factor_in[m] = factors[s, m]

            def give(j, s=s):
                elsewhere(s, members + j, final_copy(s, j).start)
                elsewhere(s, members + j, factor_copy(s, j, m).start)

            repeat(members, give)

    @pl.when(is_owner)
    def _():
        for k in range(per_owner - 1, -1, -1):
            for s in range(hosts):
                compose(k, s)
            lead(k)
        pl.when(half == 0)(front_half)
        pl.when(half == 1)(back_half)

    pl.when(is_owner)(lambda: landed(factor_in.at[pl.ds(0, owners - 1)], factor_recv_sem))
    pl.when(jnp.logical_not(is_owner))(lambda: landed(factor_in, factor_recv_sem))
    for q in range(owners):
        for h in range(HALVES):
            needed = jnp.logical_not(both(is_host, d == h * members + q))
            if h == 0:
                needed = both(needed, half == 0)
            pl.when(needed)(functools.partial(landed, pair_in.at[h, q], pair_recv_sem.at[h, q]))

        @pl.when(half == 0)
        def _(q=q):
            for k in range(per_owner):
                c = k * owners + q
                where = slice(c * LANES, (c + 1) * LANES)
                before = jnp.exp2(pair_in[0, q, k, 0])
                front_ref[0, :, where] = factor_in[q, k]
                image_ref[0, :, where] = pair_in[0, q, k, 1] + before * pair_in[1, q, k, 1]
                image_ref[1, :, where] = before * jnp.exp2(pair_in[1, q, k, 0])

        @pl.when(half == 1)
        def _(q=q):
            for k in range(per_owner):
                c = k * owners + q
                where = slice(c * LANES, (c + 1) * LANES)
                front_ref[0, :, where] = factor_in[q, k]
                image_ref[0, :, where] = pair_in[1, q, k, 0]
                image_ref[1, :, where] = pair_in[1, q, k, 1]

    pl.when(up_d)(lambda: landed(dens.at[:, 0, pl.ds(0, rows), :], depth_send_sem))
    pl.when(up_r)(lambda: landed(row_send, rows_send_sem))
    pl.when(both(up_d, up_r))(corner_copy.wait_send)
    pl.when(jnp.logical_not(is_owner))(lambda: landed(parts, part_send_sem))

    @pl.when(is_owner)
    def _():
        landed(parts.at[pl.ds(0, tiles - per_owner)], part_send_sem)
        for s in range(hosts):
            others = members
            if s == hosts - 1:
                others = members - 1
            landed(factors.at[s, pl.ds(0, others)], factor_send_sem.at[s])

            @pl.when(half == 0)
            def _(s=s):
                if s < hosts - 1:
                    landed(gathered.at[s, :, pl.ds(0, members - 1)], pair_send_sem.at[s, 0])
                else:
                    pl.when(d == 0)(
                        lambda: landed(gathered.at[s, :, pl.ds(0, members - 1)], pair_send_sem.at[s, 0])
                    )
                    pl.when(d > 0)(
                        lambda: landed(gathered.at[s, :, pl.ds(0, members - 2)], pair_send_sem.at[s, 0])
                    )
                landed(pairs.at[s], pair_send_sem.at[s, 1])

            @pl.when(half == 1)
            def _(s=s, others=others):
                landed(gathered.at[s, :, pl.ds(0, members - 1)], pair_send_sem.at[s, 0])
                landed(gathered.at[s, :, pl.ds(0, others)], pair_send_sem.at[s, 1])

        pl.when(half == 0)(led)


def on_device(n_depth, n_rows, density, bin_of_level, absorb_bins, emit_bins, occupancy, col_offsets, row_offsets):
    slab, rows, cols = density.shape
    tiles = cols // LANES
    row_tiles = rows // SUB
    members = n_depth // HALVES
    hosts = 2 if n_rows % 2 == 0 else 1
    owners = 1
    while owners * 2 <= members and tiles % (owners * 2) == 0:
        owners *= 2
    per_owner = tiles // owners
    groups = tiles // 2 if tiles % 2 == 0 else tiles
    anywhere = pl.BlockSpec(memory_space=pl.ANY)
    vmem = pl.BlockSpec(memory_space=pltpu.VMEM)
    f32, i32 = jnp.float32, jnp.int32
    dma = pltpu.SemaphoreType.DMA
    held = pl.pallas_call(
        functools.partial(kernel, n_depth, n_rows, hosts, owners),
        out_shape=(pltpu.VMEM((1, rows, cols), f32), pltpu.VMEM((2, rows, cols), f32)),
        in_specs=[anywhere] * 7,
        out_specs=(vmem, vmem),
        scratch_shapes=[
            pltpu.VMEM((tiles, slab + 1, rows + SUB, LANES), f32),
            pltpu.SMEM(bin_of_level.shape, i32),
            pltpu.SMEM(absorb_bins.shape, f32),
            pltpu.SMEM(emit_bins.shape, f32),
            pltpu.SMEM(occupancy.shape, i32),
            pltpu.VMEM((tiles, LANES), i32),
            pltpu.SMEM(row_offsets.shape, i32),
            pltpu.VMEM((tiles, slab, LANES), f32),
            pltpu.VMEM((tiles, slab, LANES), f32),
            pltpu.VMEM((tiles, LANES), f32),
            pltpu.VMEM((tiles, LANES), f32),
            pltpu.VMEM((slab, SUB, LANES), f32),
            pltpu.VMEM((row_tiles, tiles, 3, SUB, LANES), f32),
            pltpu.VMEM((tiles, 2, rows, LANES), f32),
            pltpu.VMEM((hosts, per_owner, members, 2, rows, LANES), f32),
            pltpu.VMEM((hosts, members, per_owner, rows, LANES), f32),
            pltpu.VMEM((hosts, per_owner, 2, rows, LANES), f32),
            pltpu.VMEM((hosts, per_owner, 2, rows, LANES), f32),
            pltpu.VMEM((hosts, per_owner, 2, rows, LANES), f32),
            pltpu.VMEM((owners, per_owner, rows, LANES), f32),
            pltpu.VMEM((HALVES, owners, per_owner, 2, rows, LANES), f32),
            dma,
            dma,
            dma,
            dma((6,)),
            pltpu.SemaphoreType.REGULAR,
            dma,
            dma((groups,)),
            dma,
            dma((groups,)),
            dma((2,)),
            dma,
            dma((hosts, per_owner)),
            dma((hosts,)),
            dma,
            dma((hosts, HALVES)),
            dma((HALVES, owners)),
            dma((hosts,)),
            dma((hosts,)),
        ],
        compiler_params=pltpu.CompilerParams(collective_id=0, has_side_effects=True),
    )(
        density,
        bin_of_level,
        absorb_bins,
        emit_bins,
        occupancy,
        col_offsets.reshape(tiles, LANES),
        row_offsets,
    )
    return pl.pallas_call(
        put_out,
        out_shape=(jax.ShapeDtypeStruct((1, rows, cols), f32), jax.ShapeDtypeStruct((2, rows, cols), f32)),
        in_specs=[vmem] * 2,
        out_specs=(anywhere, anywhere),
        scratch_shapes=[dma((2,))],
    )(*(pltpu.with_memory_space_constraint(x, pltpu.VMEM) for x in held))


def put_out(front, image, front_out, image_out, sem):
    copies = [
        pltpu.make_async_copy(front, front_out, sem.at[0]),
        pltpu.make_async_copy(image, image_out, sem.at[1]),
    ]
    for copy in copies:
        copy.start()
    for copy in copies:
        copy.wait()


def solution(mesh):
    placed = (P("depth", "rows", None), P(), P(), P(), P("depth", "rows", None), P(), P("rows"))
    return jax.shard_map(
        functools.partial(on_device, mesh.shape["depth"], mesh.shape["rows"]),
        mesh=mesh,
        in_specs=placed,
        out_specs=(P("depth", "rows", None), P(None, "rows", None)),
        check_vma=False,
    )
```
